32 devices in a mesh: seq: 8 (over z, x), head: 4 (over y, core).
Axes of the slice: x: 2, y: 2, z: 4, core: 2. Of those that a mesh axis runs over, the one named last changes fastest.
Arguments:
- xs: bfloat16 [8192, 4096], P('seq', 'head'), may hold values from -6 to 6
- gate_branch: bfloat16 [8192, 4096], P('seq', 'head'), may hold values from -6 to 6
- bmat: bfloat16 [8192, 128], P('seq'), may hold values from -0.375 to 0.375
- cmat: bfloat16 [8192, 128], P('seq'), may hold values from -0.375 to 0.375
- dt_code: int32 [64, 8192], P('head', 'seq'), may hold values from 1 to 32768
- resets: int32 [8192], P('seq'), may hold values 0 or 1
- decay_rate: float32 [64], P('head'), may hold values from 4.8828125e-05 to 0.08, as said below
- skip: float32 [64], P('head'), may hold values from 0.5 to 1.5
- norm_gain: float32 [4096], P('head'), may hold values from 0.1 to 1.9
- out_weight: bfloat16 [4096, 4096], P('head'), may hold values from -0.09375 to 0.09375
Outputs:
- mixed: bfloat16 [8192, 4096], P(('seq', 'head'))
The draws below stay inside these ranges and needn't reach their ends.
Inputs may be any that keep to these rules, and one draw needn't show every extreme that they name: `decay_rate`: positive rates.
All inputs are finite; a program needn't handle non-finite values. No bound on the sum of `resets` on one device may be relied on, other than what follows from the above.
Results may differ from the reference program's by a relative error of at most 0.023.
Values may be sent and summed in bfloat16 or wider, within the bound.
No kernel may reach another device: no remote copies, remote signals or barrier semaphores. Data moves between devices by JAX's collectives and lax.ppermute only.
A program may use at most 128 MiB of HBM per device.

```python
import jax
import jax.numpy as jnp
from jax import lax

D = 4096
HEADS = 64
HEAD_DIM = 64
STATE = 128
SPAN = 256
HORIZON_TICKS = 8192
INNER = 4096
GROUPS = 4


def draw_xs(key, part):
    first = jax.random.fold_in(key, 0)
    values = jax.random.normal(first, (HORIZON_TICKS, INNER), jnp.float32)
    return jnp.clip(values, -6.0, 6.0).astype(jnp.bfloat16)


def draw_dt_code(key, part):
    first, right_factor = jax.random.split(jax.random.fold_in(key, 11))
    starting_displacement = jax.random.randint(first, (HEADS, HORIZON_TICKS), 1, 17)
    contiguous_span_count = jax.random.randint(right_factor, (HORIZON_TICKS,), 0, HORIZON_TICKS) < 3
    return jnp.where(contiguous_span_count[None, :], 4 * HORIZON_TICKS, starting_displacement).astype(jnp.int32)


def draw_decay_rate(key, part):
    first, right_factor, third = jax.random.split(jax.random.fold_in(key, 23), 3)
    share = 0.5
    slow_mask = jax.random.uniform(first, (HEADS,), jnp.float32) < share
    slow_rate = jnp.exp(jax.random.uniform(right_factor, (HEADS,), jnp.float32, jnp.log(0.4), jnp.log(1.6))) / HORIZON_TICKS
    fast_rate = jnp.exp(jax.random.uniform(third, (HEADS,), jnp.float32, jnp.log(0.03), jnp.log(0.08)))
    return jnp.where(slow_mask, slow_rate, fast_rate).astype(jnp.float32)


def place_ends(drawn, key, low, high):
    longest = drawn.shape.index(max(drawn.shape))
    spots = []
    for shift in (0, 1):
        where = [jax.random.randint(jax.random.fold_in(key, axis), (), 0, length) for axis, length in enumerate(drawn.shape)]
        where[longest] = (where[longest] + shift) % drawn.shape[longest]
        spots.append(tuple(where))
    return drawn.at[spots[0]].set(low).at[spots[1]].set(high)


def shard_levels(rng, shape, shards, low, top_value):
    level, own = 1.0, jax.random.fold_in(rng, 6)
    for dim, parts in shards:
        draws = jnp.exp(jax.random.uniform(jax.random.fold_in(own, dim), (parts,), jnp.float32, low / len(shards), top_value / len(shards)))
        level = level * jnp.repeat(draws, shape[dim] // parts).reshape([-1 if axis == dim else 1 for axis in range(len(shape))])
    return level


def centred(own_key, shape, spread, reach, cuts=(), kind=jnp.bfloat16):
    entries = spread * jax.random.normal(own_key, shape, jnp.float32)
    if cuts:
        entries = entries * shard_levels(own_key, shape, cuts, -0.22, 0.18)
    return jnp.clip(entries, -reach, reach).astype(kind)


def setup_inputs(seed: int = 0) -> dict:
    key_of = jax.random.split(jax.random.key(seed), 11)
    xs = draw_xs(jax.random.fold_in(key_of[10], 71), 0)
    gate_branch = centred(key_of[1], (HORIZON_TICKS, INNER), 1.0, 6.0, ((0, 8), (1, 4)))
    bmat = centred(key_of[2], (HORIZON_TICKS, STATE), (2 * (HORIZON_TICKS * STATE) ** -0.25), 0.375, ((0, 8),))
    cmat = centred(key_of[3], (HORIZON_TICKS, STATE), (2 * (HORIZON_TICKS * STATE) ** -0.25), 0.375, ((0, 8),))
    dt_code = draw_dt_code(jax.random.fold_in(key_of[10], 71), 0)
    resets = place_ends((jax.random.randint(key_of[5], (HORIZON_TICKS,), 0, HORIZON_TICKS) < 2).astype(jnp.int32), jax.random.fold_in(key_of[5], 1), 0, 1)
    decay_rate = draw_decay_rate(jax.random.fold_in(key_of[10], 71), 0)
    skip = jnp.clip(0.5 + 1.0 * jax.random.uniform(key_of[7], (HEADS,), jnp.float32) ** shard_levels(key_of[7], (HEADS,), ((0, 4),), -0.2, 0.2), 0.5, 1.5)
    norm_gain = jnp.clip(1.0 + 0.18 * jax.random.normal(key_of[8], (INNER,), jnp.float32), 0.1, 1.9)
    out_weight = centred(key_of[9], (INNER, D), INNER ** -0.5, 0.09375, ((0, 4),))
    return {"xs": xs, "gate_branch": gate_branch, "bmat": bmat, "cmat": cmat, "dt_code": dt_code, "resets": resets, "decay_rate": decay_rate, "skip": skip, "norm_gain": norm_gain, "out_weight": out_weight}


def reference(xs, gate_branch, bmat, cmat, dt_code, resets, decay_rate, skip, norm_gain, out_weight):
    step_size = dt_code.astype(jnp.float32) / 16.0
    input_scale = jnp.minimum(step_size, 1.0)
    logarithmic_damping = -decay_rate[:, None] * step_size
    blocks = HORIZON_TICKS // SPAN
    values = xs.reshape(blocks, SPAN, HEADS, HEAD_DIM)
    key_blocks = bmat.reshape(blocks, SPAN, STATE)
    query_blocks = cmat.reshape(blocks, SPAN, STATE)
    log_blocks = logarithmic_damping.reshape(HEADS, blocks, SPAN).transpose(1, 0, 2)
    scale_blocks = input_scale.reshape(HEADS, blocks, SPAN).transpose(1, 0, 2)
    flag_blocks = resets.reshape(blocks, SPAN)

    def propagate_forward(state, inputs):
        value, key_rows, query, logs, scales, flags = inputs
        cumulative = jnp.cumsum(logs, axis=1)
        counts = jnp.cumsum(flags)
        position = jnp.arange(SPAN)
        linked = (counts[:, None] == counts[None, :]) & (position[None, :] <= position[:, None])
        gaps = jnp.where(linked[None], cumulative[:, :, None] - cumulative[:, None, :], 0.0)
        within = jnp.where(linked[None], jnp.exp(gaps), 0.0)
        intersection = jnp.dot(query, key_rows.T, preferred_element_type=jnp.float32)
        value_float = value.astype(jnp.float32)
        scaled = (value_float * scales.T[:, :, None]).astype(jnp.bfloat16)
        scaled_float = lax.optimization_barrier(scaled).astype(jnp.float32)
        scores = (within * intersection[None]).astype(jnp.bfloat16)
        scores_float = lax.optimization_barrier(scores).astype(jnp.float32)
        output = jnp.einsum('hij,jhp->ihp', scores_float, scaled_float, precision=lax.Precision.HIGHEST)
        from_start = jnp.where(counts[None, :] == 0, jnp.exp(cumulative), 0.0)
        query_float = query.astype(jnp.float32)
        carried = jnp.einsum('in,hpn->ihp', query_float, state, precision=lax.Precision.HIGHEST)
        output = output + carried * from_start.T[:, :, None]
        to_end = jnp.where(counts[None, :] == counts[-1], jnp.exp(cumulative[:, -1:] - cumulative), 0.0)
        through = jnp.where(counts[-1] == 0, jnp.exp(cumulative[:, -1]), 0.0)
        weighted = (scaled_float * to_end.T[:, :, None]).astype(jnp.bfloat16)
        weighted_float = lax.optimization_barrier(weighted).astype(jnp.float32)
        fresh = jnp.einsum('jhp,jn->hpn', weighted_float, key_rows.astype(jnp.float32), precision=lax.Precision.HIGHEST)
        state = through[:, None, None] * state + fresh
        output = output + skip[None, :, None] * value_float
        return (state, output)
    initial = jnp.zeros((HEADS, HEAD_DIM, STATE), jnp.float32)
    outputs = lax.scan(propagate_forward, initial, (values, key_blocks, query_blocks, log_blocks, scale_blocks, flag_blocks))[1]
    ssm_out = outputs.reshape(HORIZON_TICKS, INNER)
    gated = ssm_out * jax.nn.silu(gate_branch.astype(jnp.float32))
    mean_square = lax.optimization_barrier(jnp.mean(gated * gated, axis=1, keepdims=True))
    hidden = (gated * lax.rsqrt(mean_square + 1e-05) * norm_gain[None, :]).astype(jnp.bfloat16)
    group_width = INNER // GROUPS
    summed = jnp.zeros((HORIZON_TICKS, D), jnp.float32)
    for group in range(GROUPS):
        lower = group * group_width
        partial_value = jnp.dot(hidden[:, lower:lower + group_width], out_weight[lower:lower + group_width], preferred_element_type=jnp.float32).astype(jnp.bfloat16)
        summed = summed + lax.optimization_barrier(partial_value).astype(jnp.float32)
    return summed.astype(jnp.bfloat16)
```

```python
import functools

import jax
import jax.numpy as jnp
from jax import lax
from jax.experimental import pallas as pl
from jax.experimental.pallas import tpu as pltpu
from jax.sharding import PartitionSpec as P


SPAN = 256
LANES = 128
LOG2E = 1.4426950408889634
F32 = jnp.float32
BF16 = jnp.bfloat16
PARAMS = pltpu.CompilerParams(vmem_limit_bytes=24 << 20)
CUTS = (1, 3, 4, 4, 2, 2)


def block_of(place, k, teams, i):
    team = (place[0] // 2 + k) % teams
    half = place[0] % 2
    return 2 * team + (half if i == 0 else 1 - half)


def block_cumsum(v):
    pos = lax.broadcasted_iota(jnp.int32, v.shape, 1) % SPAN
    k = 1
    while k < SPAN:
        v = v + jnp.where(pos >= k, pltpu.roll(v, k, 1), 0.0)
        k *= 2
    return v


def prep(dt, rate_ref, resets):
    step = dt.astype(F32) / 16.0
    scale = jnp.minimum(step, 1.0)
    row = lax.broadcasted_iota(jnp.int32, step.shape, 0)
    rate = jnp.zeros(step.shape, F32)
    for h in range(step.shape[0]):
        rate = jnp.where(row == h, rate_ref[h], rate)
    cum = block_cumsum((-LOG2E * rate) * step)
    count = block_cumsum(jnp.broadcast_to(resets.astype(F32), (8, resets.shape[1])))
    return scale, cum, count


def halves(first, second, shape, width):
    lane = lax.broadcasted_iota(jnp.int32, shape, 1) % LANES
    return jnp.where(lane < width, first, second)


def state_kernel(dt_ref, rate_ref, resets_ref, b_ref, x_ref, pay_ref, start_ref, reach_ref, w_s, bt_s, thr_s, *, pairs, width):
    blocks = start_ref.shape[0]
    state = b_ref.shape[1]

    @pl.when(pl.program_id(0) == 0)
    def _():
        scale, cum, count = prep(dt_ref[...], rate_ref, resets_ref[...])
        heads = cum.shape[0]
        for b in range(blocks):
            cols = slice(b * SPAN, (b + 1) * SPAN)
            c, n = cum[:, cols], count[:1, cols]
            end, last = c[:, SPAN - 1 :], n[:, SPAN - 1 :]
            w_s[:, cols] = jnp.where(n == last, jnp.exp2(end - c), 0.0) * scale[:, cols]
            through = jnp.where(last == 0.0, jnp.exp2(end), 0.0)
            thr_s[:, b * LANES : (b + 1) * LANES] = jnp.broadcast_to(through, (heads, LANES))
        bt_s[...] = b_ref[...].astype(F32).T

    own = pl.ds(pl.multiple_of(pl.program_id(0) * 2 * pairs, 2 * pairs), 2 * pairs)
    for i in range(pairs):
        lanes = slice(i * LANES, (i + 1) * LANES)
        running = jnp.zeros((state, LANES), F32)
        product = jnp.ones((1, LANES), F32)
        for b in range(blocks):
            cols = slice(b * SPAN, (b + 1) * SPAN)
            start_ref[b, :, lanes] = running.astype(BF16)
            reach_ref[b, :, lanes] = jnp.broadcast_to(product, (8, LANES))
            x = x_ref[cols, lanes]
            parts = []
            for k in range(2):
                row = w_s[own, cols][2 * i + k : 2 * i + k + 1]
                left = (bt_s[:, cols] * row).astype(BF16)
                parts.append(jnp.dot(left, x, preferred_element_type=F32))
            fresh = halves(parts[0], parts[1], (state, LANES), width)
            thr = thr_s[own, b * LANES : (b + 1) * LANES]
            thr = halves(thr[2 * i : 2 * i + 1], thr[2 * i + 1 : 2 * i + 2], (1, LANES), width)
            running = thr * running + fresh
            product = product * thr
        high = product.astype(BF16).astype(F32)
        mid = (product - high).astype(BF16).astype(F32)
        low = product - high - mid
        row = lax.broadcasted_iota(jnp.int32, (16, LANES), 0)
        tail = jnp.where(row == 0, high, jnp.where(row == 1, mid, jnp.where(row == 2, low, 0.0)))
        pay_ref[i, :state, :] = running.astype(BF16)
        pay_ref[i, state:, :] = tail.astype(BF16)


def states(dt, rate, resets, bmat, xs, blocks, width, pairs=4):
    tokens, channels = xs.shape
    heads, state = dt.shape[0], bmat.shape[1]
    count = channels // LANES
    whole = lambda *shape: pl.BlockSpec(shape, lambda i: (0,) * len(shape))
    return pl.pallas_call(
        functools.partial(state_kernel, pairs=pairs, width=width),
        grid=(count // pairs,),
        in_specs=[
            whole(heads, tokens),
            pl.BlockSpec(memory_space=pltpu.SMEM),
            whole(1, tokens),
            whole(tokens, state),
            pl.BlockSpec((tokens, pairs * LANES), lambda i: (0, i)),
        ],
        out_specs=[
            pl.BlockSpec((pairs, state + 16, LANES), lambda i: (i, 0, 0)),
            pl.BlockSpec((blocks, state, pairs * LANES), lambda i: (0, 0, i)),
            pl.BlockSpec((blocks, 8, pairs * LANES), lambda i: (0, 0, i)),
        ],
        out_shape=[
            jax.ShapeDtypeStruct((count, state + 16, LANES), BF16),
            jax.ShapeDtypeStruct((blocks, state, channels), BF16),
            jax.ShapeDtypeStruct((blocks, 8, channels), F32),
        ],
        scratch_shapes=[
            pltpu.VMEM((heads, tokens), F32),
            pltpu.VMEM((state, tokens), F32),
            pltpu.VMEM((heads, blocks * LANES), F32),
        ],
        cost_estimate=pl.CostEstimate(flops=4 * tokens * channels * state, bytes_accessed=4 << 20, transcendentals=tokens * heads),
        compiler_params=PARAMS,
        name="states",
    )(dt, rate, resets, bmat, xs)


def prefix_kernel(pay_ref, out_ref):
    shards, state = out_ref.shape[:2]
    running = jnp.zeros(out_ref.shape[1:], F32)
    for s in range(shards):
        out_ref[s] = running.astype(BF16)
        tail = pay_ref[s, state:, :].astype(F32)
        decay = tail[0:1] + tail[1:2] + tail[2:3]
        running = decay * running + pay_ref[s, :state, :].astype(F32)


def prefix(pay):
    shards, rows, lanes = pay.shape
    return pl.pallas_call(
        prefix_kernel,
        out_shape=jax.ShapeDtypeStruct((shards, rows - 16, lanes), BF16),
        cost_estimate=pl.CostEstimate(flops=shards * rows * lanes * 2, bytes_accessed=1 << 19, transcendentals=0),
        compiler_params=PARAMS,
        name="prefix",
    )(pay)


def intra_kernel(list_ref, dt_ref, rate_ref, resets_ref, skip_ref, b_ref, c_ref, x_ref, g_ref, base_ref, carry_ref, *, width):
    scale, cum, count = prep(dt_ref[...], rate_ref, resets_ref[...])
    heads = cum.shape[0]
    rows = cum - jnp.log2(scale)
    start = jnp.where(count[:1] == 0.0, jnp.exp2(cum), 0.0)
    stack = [cum, start, count, jnp.zeros((LANES - 2 * heads - 8, SPAN), F32)]
    flipped = jnp.concatenate(stack, axis=0).T
    dots = lax.dot_general(c_ref[...], b_ref[...], (((1,), (1,)), ((), ())), preferred_element_type=F32)
    i = lax.broadcasted_iota(jnp.int32, (SPAN, SPAN), 0)
    j = lax.broadcasted_iota(jnp.int32, (SPAN, SPAN), 1)
    linked = (flipped[:, 2 * heads : 2 * heads + 1] == count[:1]) & (j <= i)
    dots = jnp.where(linked, dots, 0.0)
    for pair in range(heads // 2):
        lanes = slice(pair * LANES, (pair + 1) * LANES)
        x = x_ref[:, lanes]
        left, right = [], []
        for k in range(2):
            h = 2 * pair + k
            gap = jnp.minimum(flipped[:, h : h + 1] - rows[h : h + 1], 0.0)
            left.append((jnp.exp2(gap) * dots).astype(BF16))
            zero = jnp.zeros_like(x)
            right.append(halves(x, zero, x.shape, width) if k == 0 else halves(zero, x, x.shape, width))
        intra = jnp.dot(jnp.concatenate(left, axis=1), jnp.concatenate(right, axis=0), preferred_element_type=F32)
        weight = halves(skip_ref[2 * pair], skip_ref[2 * pair + 1], (1, LANES), width)
        gate = g_ref[:, lanes].astype(F32)
        gate = gate / (1.0 + jnp.exp(-gate))
        base_ref[0, :, lanes] = (intra + weight * x.astype(F32)) * gate
        h = heads + 2 * pair
        carry = halves(flipped[:, h : h + 1], flipped[:, h + 1 : h + 2], x.shape, width)
        carry_ref[0, :, lanes] = (carry * gate).astype(BF16)


def intra(place, k, teams, dt, rate, resets, skip, bmat, cmat, xs, gate, width):
    _, channels = xs.shape
    heads, state = dt.shape[0], bmat.shape[1]
    count = 2
    at = lambda i, o: block_of(o, k, teams, 0) + i * (1 - 2 * (o[0] % 2))
    row = lambda n: pl.BlockSpec((SPAN, n), lambda i, o: (at(i, o), 0))
    out = pl.BlockSpec((1, SPAN, channels), lambda i, o: (i, 0, 0))
    return pl.pallas_call(
        functools.partial(intra_kernel, width=width),
        grid_spec=pltpu.PrefetchScalarGridSpec(
            num_scalar_prefetch=1,
            grid=(count,),
            in_specs=[
                pl.BlockSpec((heads, SPAN), lambda i, o: (0, at(i, o))),
                pl.BlockSpec(memory_space=pltpu.SMEM),
                pl.BlockSpec((1, SPAN), lambda i, o: (0, at(i, o))),
                pl.BlockSpec(memory_space=pltpu.SMEM),
                row(state),
                row(state),
                row(channels),
                row(channels),
            ],
            out_specs=[out, out],
        ),
        out_shape=[
            jax.ShapeDtypeStruct((count, SPAN, channels), F32),
            jax.ShapeDtypeStruct((count, SPAN, channels), BF16),
        ],
        cost_estimate=pl.CostEstimate(
            flops=8 * count * SPAN * SPAN * channels, bytes_accessed=count << 21, transcendentals=count * heads * SPAN * SPAN
        ),
        compiler_params=PARAMS,
        name="intra",
    )(place, dt, rate, resets, skip, bmat, cmat, xs, gate)


def finish_kernel(list_ref, c_ref, start_ref, reach_ref, in_ref, base_ref, carry_ref, gain_ref, hid_ref, sq_ref, total_s):
    step = pl.program_id(0)

    @pl.when(step == 0)
    def _():
        total_s[...] = jnp.zeros(total_s.shape, F32)

    full = []
    for q in range(in_ref.shape[0]):
        lanes = slice(q * LANES, (q + 1) * LANES)
        full.append((start_ref[0, :, lanes].astype(F32) + reach_ref[0, 0:1, lanes] * in_ref[q].astype(F32)).astype(BF16))
    inter = jnp.dot(c_ref[...], jnp.concatenate(full, axis=1), preferred_element_type=F32)
    gated = base_ref[0] + carry_ref[0].astype(F32) * inter
    square = gated * gated
    total = total_s[...]
    for q in range(in_ref.shape[0]):
        total = total + square[:, q * LANES : (q + 1) * LANES]
    total_s[...] = total
    hid_ref[0] = (gated * gain_ref[0:1, :]).astype(BF16)

    @pl.when(step == pl.num_programs(0) - 1)
    def _():
        sums = jnp.sum(total_s[...].T, axis=0, keepdims=True)
        sq_ref[0] = jnp.broadcast_to(sums, (8, SPAN))


def finish(place, k, teams, which, cmat, starts, reach, incoming, base, carry, gain, pairs=2):
    channels = base.shape[2]
    state = cmat.shape[1]
    wide = pairs * LANES
    at = lambda o: block_of(o, k, teams, which)
    part = pl.BlockSpec((1, SPAN, wide), lambda i, o: (which, 0, i))
    return pl.pallas_call(
        finish_kernel,
        grid_spec=pltpu.PrefetchScalarGridSpec(
            num_scalar_prefetch=1,
            grid=(channels // wide,),
            in_specs=[
                pl.BlockSpec((SPAN, state), lambda i, o: (at(o), 0)),
                pl.BlockSpec((1, state, wide), lambda i, o: (at(o), 0, i)),
                pl.BlockSpec((1, 8, wide), lambda i, o: (at(o), 0, i)),
                pl.BlockSpec((pairs, *incoming.shape[1:]), lambda i, o: (i, 0, 0)),
                part,
                part,
                pl.BlockSpec((1, wide), lambda i, o: (0, i)),
            ],
            out_specs=[
                pl.BlockSpec((1, SPAN, wide), lambda i, o: (0, 0, i)),
                pl.BlockSpec((1, 8, SPAN), lambda i, o: (0, 0, 0)),
            ],
            scratch_shapes=[pltpu.VMEM((SPAN, LANES), F32)],
        ),
        out_shape=[
            jax.ShapeDtypeStruct((1, SPAN, channels), BF16),
            jax.ShapeDtypeStruct((1, 8, SPAN), F32),
        ],
        cost_estimate=pl.CostEstimate(flops=2 * SPAN * state * channels, bytes_accessed=3 << 20, transcendentals=0),
        compiler_params=PARAMS,
        name="finish",
    )(place, cmat, starts, reach, incoming, base, carry, gain)


def product_kernel(a_ref, b_ref, wa_ref, wb_ref, out_ref):
    total = jnp.dot(a_ref[0], wa_ref[...], preferred_element_type=F32)
    total = total + jnp.dot(b_ref[0], wb_ref[...], preferred_element_type=F32)
    out_ref[...] = total.astype(out_ref.dtype)


def product(a, b, wa, wb, first, columns, dtype, tile=256):
    rows, depth = a.shape[1:]
    left = pl.BlockSpec((1, rows, depth), lambda i: (0, 0, 0))
    right = pl.BlockSpec((depth, tile), lambda i: (0, first // tile + i))
    return pl.pallas_call(
        product_kernel,
        grid=(columns // tile,),
        in_specs=[left, left, right, right],
        out_specs=pl.BlockSpec((rows, tile), lambda i: (0, i)),
        out_shape=jax.ShapeDtypeStruct((rows, columns), dtype),
        cost_estimate=pl.CostEstimate(flops=4 * rows * depth * columns, bytes_accessed=4 * depth * columns, transcendentals=0),
        compiler_params=PARAMS,
        name="product",
    )(a, b, wa, wb)


def close(square, own, parts, inner, out, first, tile=256):
    rows, columns = parts[0].shape
    at = lambda i: (0, first // tile + i)

    def body(*refs):
        sq_ref, own_ref = refs[:2]
        part_refs = refs[2 : 2 + len(parts)]
        out_ref = refs[-1]
        row = lax.rsqrt(sq_ref[...] / inner + 1e-05)
        total = own_ref[...]
        for part in part_refs:
            total = total + part[...].astype(F32)
        out_ref[...] = (total * row.T[:, 0:1]).astype(BF16)

    in_specs = [pl.BlockSpec(square.shape, lambda i: (0, 0)), pl.BlockSpec((rows, tile), at)]
    in_specs += [pl.BlockSpec((rows, tile), lambda i: (0, i))] * len(parts)
    args = [square, own, *parts]
    aliases = {}
    if out is not None:
        in_specs.append(pl.BlockSpec(memory_space=pl.ANY))
        args.append(out)
        aliases = {len(args) - 1: 0}
    return pl.pallas_call(
        body,
        grid=(columns // tile,),
        in_specs=in_specs,
        out_specs=pl.BlockSpec((rows, tile), at),
        out_shape=jax.ShapeDtypeStruct(own.shape, BF16),
        input_output_aliases=aliases,
        cost_estimate=pl.CostEstimate(flops=4 * rows * columns, bytes_accessed=8 * rows * columns, transcendentals=0),
        compiler_params=PARAMS,
        name="close",
    )(*args)


def exchange(slices):
    return lax.all_to_all(slices, "seq", 0, 0, tiled=True)


def local(xs, gate, bmat, cmat, dt, resets, decay_rate, skip, gain, weight, *, shards, group):
    tokens, channels = xs.shape
    heads, state = dt.shape[0], bmat.shape[1]
    width = channels // heads
    blocks = tokens // SPAN
    pairs = channels // LANES
    inner = float(group * channels)
    out_columns = weight.shape[1]
    me = lax.axis_index("head")
    teams = group // 2

    place = me.reshape(1).astype(jnp.int32)
    flags, gains = resets[None, :], gain[None, :]
    swap = [(i, i ^ 1) for i in range(group)]
    weight_b = lax.ppermute(weight, "head", swap)

    xs, gate, bmat, cmat, dt, weight, weight_b = [
        pltpu.with_memory_space_constraint(a, pltpu.HBM) for a in (xs, gate, bmat, cmat, dt, weight, weight_b)
    ]

    def after(value, *others):
        return lax.optimization_barrier((value, *others))[0]

    def inside(k, when):
        parts = intra(when, k, teams, dt, decay_rate, flags, skip, bmat, cmat, xs, gate, width)
        return [pltpu.with_memory_space_constraint(a, pltpu.HBM) for a in parts]

    payload, starts, reach = states(dt, decay_rate, flags, bmat, xs, blocks, width)
    rows = state + 16
    cut = channels // shards
    plain = shards == pairs
    if not plain:
        payload = payload.transpose(1, 0, 2).reshape(rows, shards, cut).transpose(1, 0, 2)
    gathered = exchange(payload)
    early = after(place, payload)
    locals_ = {k: inside(k, early) for k in range(1, teams)}
    prefixes = prefix(gathered)
    incoming = exchange(prefixes)
    locals_[0] = inside(0, after(place, prefixes))
    if not plain:
        incoming = incoming.transpose(1, 0, 2).reshape(state, pairs, LANES).transpose(1, 0, 2)

    def pair_of(k, when):
        done = []
        for which in (1, 0):
            hidden, sq = finish(when, k, teams, which, cmat, starts, reach, incoming, *locals_[k], gains)
            done.append((hidden, sq[0]))
        other = lax.ppermute(done[0][0], "head", swap)
        square = done[1][1] + lax.ppermute(done[0][1], "head", swap)
        return done[1][0], other, square

    received = []
    squares = []
    last = place
    unit = out_columns // sum(CUTS)
    for k in [*range(1, teams), 0]:
        hidden, other, square = pair_of(k, last)
        if k:
            send = [(i, (i + 2 * k) % group) for i in range(group)]
            squares.append(lax.ppermute(square, "head", send))
            first = 0
            chunks = []
            for n in CUTS:
                part = product(hidden, other, weight, weight_b, first, n * unit, BF16)
                hidden, part = lax.optimization_barrier((hidden, part))
                chunks.append(lax.ppermute(part, "head", send))
                first += n * unit
            last = after(place, part)
            received.append(chunks)
        else:
            squares.append(square)
            own = product(hidden, other, weight, weight_b, 0, out_columns, F32)
    square = sum(squares[1:], squares[0])
    out, first = None, 0
    for c, n in enumerate(CUTS):
        parts = [r[c] for r in received]
        out = close(square, own, parts, inner, out, first)
        if c + 1 < len(CUTS):
            for r in received:
                out, r[c + 1] = lax.optimization_barrier((out, r[c + 1]))
        first += n * unit
    return out


def solution(mesh):
    in_specs = (
        P("seq", "head"),
        P("seq", "head"),
        P("seq", None),
        P("seq", None),
        P("head", "seq"),
        P("seq"),
        P("head"),
        P("head"),
        P("head"),
        P("head", None),
    )
    out_specs = P(("seq", "head"), None)
    body = functools.partial(local, shards=mesh.shape["seq"], group=mesh.shape["head"])

    return jax.shard_map(body, mesh=mesh, in_specs=in_specs, out_specs=out_specs, check_vma=False)
```

```python
import functools

import jax
import jax.numpy as jnp
from jax import lax
from jax.experimental import pallas as pl
from jax.experimental.pallas import tpu as pltpu
from jax.sharding import PartitionSpec as P


SPAN = 256
LANES = 128
LOG2E = 1.4426950408889634
F32 = jnp.float32
BF16 = jnp.bfloat16
PARAMS = pltpu.CompilerParams(vmem_limit_bytes=24 << 20)
WHOLE = pltpu.CompilerParams(vmem_limit_bytes=60 * 1024 * 1024)
CUTS = (1, 3, 5, 3, 3, 1)
ALONE = 3
TAIL = 8
RING = 4


def block_of(place, k, teams, i):
    team = (place[0] // 2 + k) % teams
    half = place[0] % 2
    return 2 * team + (half if i == 0 else 1 - half)


def block_cumsum(v):
    pos = lax.broadcasted_iota(jnp.int32, v.shape, 1) % SPAN
    k = 1
    while k < SPAN:
        v = v + jnp.where(pos >= k, pltpu.roll(v, k, 1), 0.0)
        k *= 2
    return v


def column_of(row):
    n = row.shape[1]
    at = lax.broadcasted_iota(jnp.int32, (n, n), 0) == lax.broadcasted_iota(jnp.int32, (n, n), 1)
    return jnp.sum(jnp.where(at, jnp.broadcast_to(row, (n, n)), 0.0), axis=1, keepdims=True)


def where_am_i():
    shard = lax.axis_index("seq")
    return lax.axis_index("head"), shard & (RING - 1), shard >> (RING.bit_length() - 1)


def prep(dt, rate, resets):
    step = dt.astype(F32) / 16.0
    scale = jnp.minimum(step, 1.0)
    cum = block_cumsum((-LOG2E * column_of(rate)) * step)
    count = block_cumsum(jnp.broadcast_to(resets.astype(F32), (8, resets.shape[1])))
    return scale, cum, count


def halves(first, second, shape, width):
    lane = lax.broadcasted_iota(jnp.int32, shape, 1) % LANES
    return jnp.where(lane < width, first, second)


def fetch(sems, pairs):
    copies = [pltpu.make_async_copy(src, dst, sems.at[i]) for i, (src, dst) in enumerate(pairs)]
    for copy in copies:
        copy.start()
    return copies


def state_kernel(rate_any, skip_any, dt_any, resets_any, b_any, c_any, x_any, *refs, width):
    place_ref = where_am_i()
    pay_refs, tables, scratch = refs[:RING], refs[RING : RING + 8], refs[RING + 8 :]
    start_ref, reach_ref, b_ref, c_ref, row_ref, count_ref, flip_ref, skip_ref = tables
    rate_s, skip_s, dt_s, resets_s, x_s, w_s, bt_s, thr_s, sems = scratch
    blocks, state, channels = start_ref.shape
    wide = channels // RING
    pairs = wide // LANES
    quarters = [place_ref[1] ^ k for k in range(RING)]
    moves = [(dt_any, dt_s), (resets_any, resets_s), (rate_any, rate_s), (skip_any, skip_s), (b_any, b_ref)]
    moves += [(x_any.at[:, pl.ds(pl.multiple_of(q * wide, wide), wide)], x_s.at[k]) for k, q in enumerate(quarters)]
    moves.append((c_any, c_ref))
    copies = fetch(sems, moves)
    for copy in copies[:4]:
        copy.wait()
    scale, cum, count = prep(dt_s[...], rate_s[...], resets_s[...])
    heads = cum.shape[0]
    for b in range(blocks):
        cols = slice(b * SPAN, (b + 1) * SPAN)
        c, n = cum[:, cols], count[:1, cols]
        end, last = c[:, SPAN - 1 :], n[:, SPAN - 1 :]
        w_s[:, cols] = jnp.where(n == last, jnp.exp2(end - c), 0.0) * scale[:, cols]
        through = jnp.where(last == 0.0, jnp.exp2(end), 0.0)
        thr_s[:, b * LANES : (b + 1) * LANES] = jnp.broadcast_to(through, (heads, LANES))
    copies[4].wait()
    bt_s[...] = b_ref[...].astype(F32).T
    two = 4 * pairs
    for k, quarter in enumerate(quarters):
        own = pl.ds(pl.multiple_of(quarter // 2 * two, two), two)
        odd = quarter % 2 == 1

        def rows_of(ref, cols):
            both = ref[own, cols]
            return jnp.where(odd, both[two // 2 :], both[: two // 2])

        copies[5 + k].wait()
        for i in range(pairs):
            lanes = pl.ds(pl.multiple_of(quarter * wide + i * LANES, LANES), LANES)
            running = jnp.zeros((state, LANES), F32)
            product = jnp.ones((1, LANES), F32)
            for b in range(blocks):
                cols = slice(b * SPAN, (b + 1) * SPAN)
                start_ref[b, :, lanes] = running.astype(BF16)
                reach_ref[b, :, lanes] = jnp.broadcast_to(product, (8, LANES))
                x = x_s[k, cols, i * LANES : (i + 1) * LANES]
                rows = rows_of(w_s, cols)
                parts = []
                for j in range(2):
                    left = (bt_s[:, cols] * rows[2 * i + j : 2 * i + j + 1]).astype(BF16)
                    parts.append(jnp.dot(left, x, preferred_element_type=F32))
                fresh = halves(parts[0], parts[1], (state, LANES), width)
                thr = rows_of(thr_s, slice(b * LANES, (b + 1) * LANES))
                thr = halves(thr[2 * i : 2 * i + 1], thr[2 * i + 1 : 2 * i + 2], (1, LANES), width)
                running = thr * running + fresh
                product = product * thr
            pay_refs[k][i, :state, :] = running.astype(BF16)
            pay_refs[k][i, state:, :] = split(product)
    row_ref[...] = cum - jnp.log2(scale)
    count_ref[...] = count
    skip_ref[...] = jnp.broadcast_to(column_of(skip_s[...]), (heads, LANES))
    start = jnp.where(count[:1] == 0.0, jnp.exp2(cum), 0.0)
    for b in range(blocks):
        cols = slice(b * SPAN, (b + 1) * SPAN)
        stack = [cum[:, cols], start[:, cols], count[:, cols], jnp.zeros((LANES - 2 * heads - 8, SPAN), F32)]
        flip_ref[b] = jnp.concatenate(stack, axis=0).T
    copies[5 + RING].wait()


def split(product):
    high = product.astype(BF16).astype(F32)
    mid = (product - high).astype(BF16).astype(F32)
    low = product - high - mid
    row = lax.broadcasted_iota(jnp.int32, (TAIL, LANES), 0)
    tail = jnp.where(row == 0, high, jnp.where(row == 1, mid, jnp.where(row == 2, low, 0.0)))
    return tail.astype(BF16)


def joined(tail):
    tail = tail.astype(F32)
    return tail[0:1] + tail[1:2] + tail[2:3]


VECTORS = pl.BlockSpec(memory_space=pltpu.VMEM)
ANYWHERE = pl.BlockSpec(memory_space=pl.ANY)


def states(dt, rate, skip, resets, bmat, cmat, xs, blocks, width):
    tokens, channels = xs.shape
    heads, state = dt.shape[0], bmat.shape[1]
    wide = channels // RING
    pay = (wide // LANES, state + TAIL, LANES)
    return pl.pallas_call(
        functools.partial(state_kernel, width=width),
        in_specs=[ANYWHERE] * 7,
        out_specs=[VECTORS] * (RING + 8),
        scratch_shapes=[
            pltpu.VMEM((1, heads), F32),
            pltpu.VMEM((1, heads), F32),
            pltpu.VMEM((heads, tokens), jnp.int32),
            pltpu.VMEM((1, tokens), jnp.int32),
            pltpu.VMEM((RING, tokens, wide), BF16),
            pltpu.VMEM((heads, tokens), F32),
            pltpu.VMEM((state, tokens), F32),
            pltpu.VMEM((heads, blocks * LANES), F32),
            pltpu.SemaphoreType.DMA((6 + RING,)),
        ],
        out_shape=[
            *[jax.ShapeDtypeStruct(pay, BF16)] * RING,
            jax.ShapeDtypeStruct((blocks, state, channels), BF16),
            jax.ShapeDtypeStruct((blocks, 8, channels), F32),
            jax.ShapeDtypeStruct((tokens, state), BF16),
            jax.ShapeDtypeStruct((tokens, state), BF16),
            jax.ShapeDtypeStruct((heads, tokens), F32),
            jax.ShapeDtypeStruct((8, tokens), F32),
            jax.ShapeDtypeStruct((blocks, SPAN, LANES), F32),
            jax.ShapeDtypeStruct((heads, LANES), F32),
        ],
        cost_estimate=pl.CostEstimate(flops=4 * tokens * channels * state, bytes_accessed=4 << 20, transcendentals=tokens * heads),
        compiler_params=PARAMS,
        name="states",
    )(rate, skip, dt, resets, bmat, cmat, xs)


def swapped(items, mine):
    a, b, c, d = items
    odd, high = mine % 2 == 1, mine // 2 == 1
    a, b, c, d = jnp.where(odd, b, a), jnp.where(odd, a, b), jnp.where(odd, d, c), jnp.where(odd, c, d)
    return jnp.where(high, c, a), jnp.where(high, d, b), jnp.where(high, a, c), jnp.where(high, b, d)


def prefix_kernel(*refs):
    pays, (total_ref, before_ref, reach_ref) = refs[:RING], refs[RING:]
    pairs, rows, _ = total_ref.shape
    state = rows - TAIL
    mine = where_am_i()[1]
    for i in range(pairs):
        items = swapped([p[i].astype(F32) for p in pays], mine)
        running = jnp.zeros((state, LANES), F32)
        product = jnp.ones((1, LANES), F32)
        before, reach = [], []
        for item in items:
            before.append(running)
            reach.append(jnp.broadcast_to(product, (8, LANES)))
            decay = joined(item[state:])
            running = decay * running + item[:state]
            product = decay * product
        for k, (first, second) in enumerate(zip(swapped(before, mine), swapped(reach, mine))):
            before_ref[k, i] = first
            reach_ref[k, i] = second
        total_ref[i, :state, :] = running.astype(BF16)
        total_ref[i, state:, :] = split(product)


def prefix(pays):
    pairs, rows, _ = pays[0].shape
    return pl.pallas_call(
        prefix_kernel,
        in_specs=[VECTORS] * RING,
        out_shape=[
            jax.ShapeDtypeStruct((pairs, rows, LANES), BF16),
            jax.ShapeDtypeStruct((RING, pairs, rows - TAIL, LANES), F32),
            jax.ShapeDtypeStruct((RING, pairs, 8, LANES), F32),
        ],
        cost_estimate=pl.CostEstimate(flops=1 << 20, bytes_accessed=1 << 19, transcendentals=0),
        compiler_params=PARAMS,
        name="prefix",
    )(*pays)


def spread_kernel(left_ref, before_ref, reach_ref, *outs, always):
    for k, out_ref in enumerate(outs):
        for i in range(out_ref.shape[0]):
            left = left_ref[i, : out_ref.shape[1], :].astype(F32)
            if not always:
                left = jnp.where(where_am_i()[2] % 2 == 1, left, 0.0)
            out_ref[i] = (before_ref[k, i] + reach_ref[k, i, 0:1, :] * left).astype(BF16)


def spread(left, before, reach, always):
    shape = before.shape[1:]
    vmem = pl.BlockSpec(memory_space=pltpu.VMEM)
    return pl.pallas_call(
        functools.partial(spread_kernel, always=always),
        in_specs=[vmem, vmem, vmem],
        out_shape=[jax.ShapeDtypeStruct(shape, BF16)] * RING,
        cost_estimate=pl.CostEstimate(flops=1 << 20, bytes_accessed=1 << 19, transcendentals=0),
        compiler_params=PARAMS,
        name="spread",
    )(left, before, reach)


def across(total, rings):
    state = total.shape[1] - TAIL
    shards = RING * rings
    level, send, gone, reach = 1, total, None, None
    while level < rings:
        got = lax.ppermute(send, "seq", [(i, i ^ (RING * level)) for i in range(shards)])
        if rings == 2:
            return got
        later = (where_am_i()[2] // level) % 2 == 1
        wide = lambda a: (a[:, :state].astype(F32), a[:, state : state + 3].astype(F32).sum(axis=1, keepdims=True))
        (mine, mine_p), (other, other_p) = wide(send), wide(got)
        if gone is None:
            gone, reach = jnp.zeros_like(mine), jnp.ones_like(mine_p)
        gone = jnp.where(later, gone + reach * other, gone)
        reach = jnp.where(later, reach * other_p, reach)
        both = jnp.where(later, mine + mine_p * other, other + other_p * mine)
        tail = (mine_p * other_p).astype(F32)
        high = lax.reduce_precision(tail, 8, 7)
        mid = lax.reduce_precision(tail - high, 8, 7)
        low = tail - high - mid
        rest = jnp.zeros((tail.shape[0], TAIL - 3, LANES), F32)
        send = jnp.concatenate([both, high, mid, low, rest], axis=1).astype(BF16)
        level *= 2
    pad = jnp.zeros((gone.shape[0], TAIL, LANES), F32)
    return jnp.concatenate([gone, pad], axis=1).astype(BF16)


def intra_kernel(skip_ref, b_ref, c_ref, row_ref, count_ref, flip_ref, x_any, g_any, w_any, *refs, k, teams, which, width):
    *outs, x_ref, g_ref, sems = refs
    base_ref, carry_ref = outs[:2]
    block = block_of(where_am_i(), k, teams, which)
    at = pl.ds(pl.multiple_of(block * SPAN, SPAN), SPAN)
    wide = x_ref.shape[1] // RING
    moves = []
    for i in range(RING):
        lanes = slice(i * wide, (i + 1) * wide)
        moves += [(x_any.at[at, lanes], x_ref.at[:, lanes]), (g_any.at[at, lanes], g_ref.at[:, lanes])]
    for out in outs[2:]:
        moves.append((w_any.at[:, : out.shape[1]], out))
    copies = fetch(sems, moves)
    rows, count, flipped = row_ref[:, at], count_ref[:, at], flip_ref[block]
    heads = rows.shape[0]
    dots = lax.dot_general(c_ref[at, :], b_ref[at, :], (((1,), (1,)), ((), ())), preferred_element_type=F32)
    i = lax.broadcasted_iota(jnp.int32, (SPAN, SPAN), 0)
    j = lax.broadcasted_iota(jnp.int32, (SPAN, SPAN), 1)
    linked = (flipped[:, 2 * heads : 2 * heads + 1] == count[:1]) & (j <= i)
    dots = jnp.where(linked, dots, 0.0)
    for pair in range(heads // 2):
        lanes = slice(pair * LANES, (pair + 1) * LANES)
        if pair * LANES % wide == 0:
            for copy in copies[2 * (pair * LANES // wide) :][:2]:
                copy.wait()
        x = x_ref[:, lanes]
        left, right = [], []
        for k in range(2):
            h = 2 * pair + k
            gap = jnp.minimum(flipped[:, h : h + 1] - rows[h : h + 1], 0.0)
            left.append((jnp.exp2(gap) * dots).astype(BF16))
            zero = jnp.zeros_like(x)
            right.append(halves(x, zero, x.shape, width) if k == 0 else halves(zero, x, x.shape, width))
        intra = jnp.dot(jnp.concatenate(left, axis=1), jnp.concatenate(right, axis=0), preferred_element_type=F32)
        weight = halves(skip_ref[2 * pair : 2 * pair + 1], skip_ref[2 * pair + 1 : 2 * pair + 2], (1, LANES), width)
        gate = g_ref[:, lanes].astype(F32)
        gate = gate / (1.0 + jnp.exp(-gate))
        base_ref[:, lanes] = (intra + weight * x.astype(F32)) * gate
        h = heads + 2 * pair
        carry = halves(flipped[:, h : h + 1], flipped[:, h + 1 : h + 2], x.shape, width)
        carry_ref[:, lanes] = (carry * gate).astype(BF16)
    for copy in copies[2 * RING :]:
        copy.wait()


def intra(k, teams, which, tables, xs, gate, weight, columns, width):
    channels = xs.shape[1]
    heads = tables[0].shape[0]
    extra = [jax.ShapeDtypeStruct((weight.shape[0], columns), BF16)] if columns else []
    return pl.pallas_call(
        functools.partial(intra_kernel, k=k, teams=teams, which=which, width=width),
        in_specs=[VECTORS] * 6 + [ANYWHERE] * 3,
        out_specs=[VECTORS] * (2 + len(extra)),
        scratch_shapes=[
            pltpu.VMEM((SPAN, channels), BF16),
            pltpu.VMEM((SPAN, channels), BF16),
            pltpu.SemaphoreType.DMA((2 * RING + len(extra),)),
        ],
        out_shape=[jax.ShapeDtypeStruct((SPAN, channels), F32), jax.ShapeDtypeStruct((SPAN, channels), BF16), *extra],
        cost_estimate=pl.CostEstimate(
            flops=8 * SPAN * SPAN * channels, bytes_accessed=2 << 20, transcendentals=heads * SPAN * SPAN
        ),
        compiler_params=PARAMS,
        name="intra",
    )(*tables, xs, gate, weight)


def finish_kernel(base_ref, carry_ref, c_ref, start_ref, reach_ref, gain_ref, *refs, k, teams, which):
    place_ref = where_am_i()
    in_refs, (hid_ref, sq_ref) = refs[:RING], refs[RING:]
    block = block_of(place_ref, k, teams, which)
    query = c_ref[pl.ds(pl.multiple_of(block * SPAN, SPAN), SPAN), :]
    pairs = in_refs[0].shape[0]
    wide = pairs * LANES
    total = jnp.zeros((SPAN, LANES), F32)
    quarters = [jnp.concatenate([r[i] for i in range(pairs)], axis=1).astype(F32) for r in in_refs]
    for q, incoming in enumerate(swapped(quarters, place_ref[1])):
        lanes = slice(q * wide, (q + 1) * wide)
        full = start_ref[block, :, lanes].astype(F32) + reach_ref[block, 0:1, lanes] * incoming
        inter = jnp.dot(query, full.astype(BF16), preferred_element_type=F32)
        gated = base_ref[:, lanes] + carry_ref[:, lanes].astype(F32) * inter
        square = gated * gated
        for i in range(pairs):
            total = total + square[:, i * LANES : (i + 1) * LANES]
        hid_ref[:, lanes] = (gated * gain_ref[0:1, lanes]).astype(BF16)
    sums = jnp.sum(total.T, axis=0, keepdims=True)
    sq_ref[...] = jnp.broadcast_to(sums, (8, SPAN))


def finish(k, teams, which, locals_, cmat, starts, reach, gain, incoming):
    channels = gain.shape[1]
    state = incoming[0].shape[1]
    return pl.pallas_call(
        functools.partial(finish_kernel, k=k, teams=teams, which=which),
        in_specs=[VECTORS] * (6 + RING),
        out_specs=[VECTORS] * 2,
        out_shape=[
            jax.ShapeDtypeStruct((SPAN, channels), BF16),
            jax.ShapeDtypeStruct((8, SPAN), F32),
        ],
        cost_estimate=pl.CostEstimate(flops=2 * SPAN * state * channels, bytes_accessed=3 << 20, transcendentals=0),
        compiler_params=PARAMS,
        name="finish",
    )(*locals_, cmat, starts, reach, gain, *incoming)


def product_kernel(*refs, count):
    wa, wb = refs[2 * count][...], refs[2 * count + 1][...]
    for i in range(count):
        total = jnp.dot(refs[2 * i][...], wa, preferred_element_type=F32)
        total = total + jnp.dot(refs[2 * i + 1][...], wb, preferred_element_type=F32)
        out_ref = refs[2 * count + 2 + i]
        out_ref[...] = total.astype(out_ref.dtype)


def product(lefts, dtypes, wa, wb, first, columns, tile):
    rows, depth = lefts[0][0].shape
    count = len(lefts)
    left = pl.BlockSpec((rows, depth), lambda i: (0, 0))
    right = pl.BlockSpec((depth, tile), lambda i: (0, first // tile + i))
    return pl.pallas_call(
        functools.partial(product_kernel, count=count),
        grid=(columns // tile,),
        in_specs=[left, left] * count + [right, right],
        out_specs=[pl.BlockSpec((rows, tile), lambda i: (0, i))] * count,
        out_shape=[jax.ShapeDtypeStruct((rows, columns), dtype) for dtype in dtypes],
        cost_estimate=pl.CostEstimate(
            flops=4 * count * rows * depth * columns, bytes_accessed=4 * depth * columns, transcendentals=0
        ),
        compiler_params=PARAMS,
        name="product",
    )(*(a for pair in lefts for a in pair), wa, wb)


def first_kernel(a_ref, b_ref, wa_ref, wb_any, out_ref, w_s, sems, *, step):
    depth, columns = w_s.shape
    parts = [slice(i, i + step) for i in range(0, depth, step)]
    copies = fetch(sems, [(wb_any.at[part, :columns], w_s.at[part]) for part in parts])
    total = jnp.dot(a_ref[...], wa_ref[...], preferred_element_type=F32)
    for copy, part in zip(copies, parts):
        copy.wait()
        total = total + jnp.dot(b_ref[:, part], w_s[part], preferred_element_type=F32)
    out_ref[...] = total.astype(out_ref.dtype)


def first_product(a, b, wa, wb, step=512):
    rows, depth = a.shape
    columns = wa.shape[1]
    return pl.pallas_call(
        functools.partial(first_kernel, step=step),
        in_specs=[VECTORS] * 3 + [ANYWHERE],
        out_specs=VECTORS,
        out_shape=jax.ShapeDtypeStruct((rows, columns), BF16),
        scratch_shapes=[pltpu.VMEM((depth, columns), BF16), pltpu.SemaphoreType.DMA((depth // step,))],
        cost_estimate=pl.CostEstimate(flops=4 * rows * depth * columns, bytes_accessed=4 * depth * columns, transcendentals=0),
        compiler_params=PARAMS,
        name="first",
    )(a, b, wa, wb)


def close(square, own, parts, inner, out, first, columns, shape, step=256):
    rows = shape[0]

    def body(*refs):
        sq_ref, own_ref = refs[:2]
        part_refs = refs[2 : 2 + len(parts)]
        out_any, made_s, sems = refs[-3:]
        row = lax.rsqrt(sq_ref[...] / inner + 1e-05).T[:, 0:1]
        copies = []
        for i in range(columns // step):
            here = slice(i * step, (i + 1) * step)
            total = own_ref[:, here]
            for part in part_refs:
                total = total + part[:, here].astype(F32)
            made_s[:, here] = (total * row).astype(BF16)
            there = slice(first + i * step, first + (i + 1) * step)
            copies.append(pltpu.make_async_copy(made_s.at[:, here], out_any.at[:, there], sems.at[i]))
            copies[-1].start()
        for copy in copies:
            copy.wait()

    args = [square, own, *parts]
    in_specs = [VECTORS] * len(args)
    aliases = {}
    if out is not None:
        in_specs.append(ANYWHERE)
        args.append(out)
        aliases = {len(args) - 1: 0}
    return pl.pallas_call(
        body,
        in_specs=in_specs,
        out_specs=ANYWHERE,
        out_shape=jax.ShapeDtypeStruct(shape, BF16),
        scratch_shapes=[pltpu.VMEM((rows, columns), BF16), pltpu.SemaphoreType.DMA((columns // step,))],
        input_output_aliases=aliases,
        cost_estimate=pl.CostEstimate(flops=4 * rows * columns, bytes_accessed=8 * rows * columns, transcendentals=0),
        compiler_params=PARAMS,
        name="close",
    )(*args)


def local(xs, gate, bmat, cmat, dt, resets, decay_rate, skip, gain, weight, *, shards, group):
    tokens, channels = xs.shape
    heads = dt.shape[0]
    width = channels // heads
    blocks = tokens // SPAN
    inner = float(group * channels)
    out_columns = weight.shape[1]
    teams = group // 2
    rings = shards // RING

    swap = [(i, i ^ 1) for i in range(group)]
    unit = out_columns // sum(CUTS)
    raw = weight
    held = (xs, gate, bmat, cmat, dt, weight, decay_rate[None, :], skip[None, :], resets[None, :])
    held = [pltpu.with_memory_space_constraint(a, pltpu.HBM) for a in held]
    xs, gate, bmat, cmat, dt, weight, decay_rate, skip, flags = held
    gains = gain[None, :]

    def after(value, *others):
        return lax.optimization_barrier((value, *others))[0]

    def inside(k, which, when):
        columns = CUTS[0] * unit if (k, which) == (0, 1) else 0
        return intra(k, teams, which, (when, *tables), xs, gate, weight, columns, width)

    def around(items):
        got = [items[0]]
        for k in range(1, RING):
            got.append(lax.ppermute(items[k], "seq", [(i, i ^ k) for i in range(shards)]))
        return got

    *pays, starts, reach, keys, queries, row, count, flip, direct = states(
        dt, decay_rate, skip, flags, bmat, cmat, xs, blocks, width
    )
    tables = (keys, queries, row, count, flip)
    weight_b = lax.ppermute(after(raw, pays[0]), "head", swap)
    gathered = around(pays)
    locals_ = {}
    early = after(direct, pays[0])
    for k in range(1, teams):
        locals_[k, 1] = inside(k, 1, early)
    total, before, ahead = prefix(gathered)
    left = across(total, rings)
    early = after(direct, total)
    for k in range(1, teams):
        locals_[k, 0] = inside(k, 0, early)
    outgoing = spread(left, before, ahead, rings > 2)
    incoming = around(outgoing)
    *locals_[0, 1], ready = inside(0, 1, after(direct, outgoing[0]))

    def pair_of(k, when):
        done = []
        late = after(gains, when)
        for which in (1, 0):
            if (k, which) not in locals_:
                locals_[k, which] = inside(k, which, when)
            hidden, sq = finish(k, teams, which, locals_[k, which], queries, starts, reach, late, incoming)
            done.append((hidden, sq))
        other = lax.ppermute(done[0][0], "head", swap)
        square = done[1][1] + lax.ppermute(done[0][1], "head", swap)
        return done[1][0], other, square

    places = [sum(CUTS[:c]) * unit for c in range(len(CUTS) + 1)]
    received = [[] for _ in CUTS]
    squares = []
    owns = {}
    mine, last = None, direct
    for k in range(1, teams):
        hidden, other, square = pair_of(k, last)
        send = [(i, (i + 2 * k) % group) for i in range(group)]
        squares.append(lax.ppermute(square, "head", send))
        for c, n in enumerate(CUTS):
            if c == ALONE and mine is None:
                *mine, square = pair_of(0, last)
                squares.append(square)
            both = c >= ALONE and k == 1
            if c == 0:
                made = [first_product(hidden, other, ready, weight_b)]
            else:
                made = product(
                    [(hidden, other), mine] if both else [(hidden, other)],
                    [BF16, F32] if both else [BF16],
                    weight,
                    weight_b,
                    places[c],
                    n * unit,
                    unit,
                )
            hidden, made = lax.optimization_barrier((hidden, made))
            if both:
                owns[c] = made[1]
            received[c].append(lax.ppermute(made[0], "head", send))
            last = after(direct, made[0])
    mine, _ = lax.optimization_barrier((mine, made[0]))
    early = product([mine], [F32], weight, weight_b, 0, places[ALONE], places[ALONE] // 3)[0]
    square = sum(squares[1:], squares[0])
    out = None
    for c, n in enumerate(CUTS):
        own = early[:, places[c] : places[c + 1]] if c < ALONE else owns[c]
        out = close(square, own, received[c], inner, out, places[c], n * unit, (SPAN, out_columns))
        if c + 1 < len(CUTS):
            out, received[c + 1] = lax.optimization_barrier((out, received[c + 1]))
    return out


def solution(mesh):
    in_specs = (
        P("seq", "head"),
        P("seq", "head"),
        P("seq", None),
        P("seq", None),
        P("head", "seq"),
        P("seq"),
        P("head"),
        P("head"),
        P("head"),
        P("head", None),
    )
    out_specs = P(("seq", "head"), None)
    body = functools.partial(local, shards=mesh.shape["seq"], group=mesh.shape["head"])

    return jax.shard_map(body, mesh=mesh, in_specs=in_specs, out_specs=out_specs, check_vma=False)
```

```python
import functools

import jax
import jax.numpy as jnp
from jax import lax
from jax.experimental import pallas as pl
from jax.experimental.pallas import tpu as pltpu
from jax.sharding import PartitionSpec as P


SPAN = 256
LANES = 128
LOG2E = 1.4426950408889634
F32 = jnp.float32
BF16 = jnp.bfloat16
PARAMS = pltpu.CompilerParams(vmem_limit_bytes=24 << 20)
WHOLE = pltpu.CompilerParams(vmem_limit_bytes=60 * 1024 * 1024)
CUTS = (2, 4, 3, 3, 3, 1)
ALONE = 3
TAIL = 8
RING = 4


def block_of(place, k, teams, i):
    team = (place[0] // 2 + k) % teams
    half = place[0] % 2
    return 2 * team + (half if i == 0 else 1 - half)


def block_cumsum(v):
    pos = lax.broadcasted_iota(jnp.int32, v.shape, 1) % SPAN
    k = 1
    while k < SPAN:
        v = v + jnp.where(pos >= k, pltpu.roll(v, k, 1), 0.0)
        k *= 2
    return v


def column_of(row):
    n = row.shape[1]
    at = lax.broadcasted_iota(jnp.int32, (n, n), 0) == lax.broadcasted_iota(jnp.int32, (n, n), 1)
    return jnp.sum(jnp.where(at, jnp.broadcast_to(row, (n, n)), 0.0), axis=1, keepdims=True)


def where_am_i():
    shard = lax.axis_index("seq")
    return lax.axis_index("head"), shard & (RING - 1), shard >> (RING.bit_length() - 1)


def prep(dt, rate, resets):
    step = dt.astype(F32) / 16.0
    scale = jnp.minimum(step, 1.0)
    cum = block_cumsum((-LOG2E * column_of(rate)) * step)
    count = block_cumsum(jnp.broadcast_to(resets.astype(F32), (8, resets.shape[1])))
    return scale, cum, count


def halves(first, second, shape, width):
    lane = lax.broadcasted_iota(jnp.int32, shape, 1) % LANES
    return jnp.where(lane < width, first, second)


def fetch(sems, pairs):
    copies = [pltpu.make_async_copy(src, dst, sems.at[i]) for i, (src, dst) in enumerate(pairs)]
    for copy in copies:
        copy.start()
    return copies


def fetch(sems, pairs):
    copies = [pltpu.make_async_copy(src, dst, sems.at[i]) for i, (src, dst) in enumerate(pairs)]
    for copy in copies:
        copy.start()
    return copies


def quarter_states(quarter, x_ref, pay_ref, start_ref, reach_ref, w_ref, bt_ref, thr_ref, width):
    blocks, state, channels = start_ref.shape
    wide = channels // RING
    pairs = wide // LANES
    two = 4 * pairs
    own = pl.ds(pl.multiple_of(quarter // 2 * two, two), two)
    odd = quarter % 2 == 1

    def rows_of(ref, cols):
        both = ref[own, cols]
        return jnp.where(odd, both[two // 2 :], both[: two // 2])

    for i in range(pairs):
        lanes = pl.ds(pl.multiple_of(quarter * wide + i * LANES, LANES), LANES)
        running = jnp.zeros((state, LANES), F32)
        product = jnp.ones((1, LANES), F32)
        for b in range(blocks):
            cols = slice(b * SPAN, (b + 1) * SPAN)
            start_ref[b, :, lanes] = running.astype(BF16)
            reach_ref[b, :, lanes] = jnp.broadcast_to(product, (8, LANES))
            x = x_ref[cols, i * LANES : (i + 1) * LANES]
            rows = rows_of(w_ref, cols)
            parts = []
            for j in range(2):
                left = (bt_ref[:, cols] * rows[2 * i + j : 2 * i + j + 1]).astype(BF16)
                parts.append(jnp.dot(left, x, preferred_element_type=F32))
            fresh = halves(parts[0], parts[1], (state, LANES), width)
            thr = rows_of(thr_ref, slice(b * LANES, (b + 1) * LANES))
            thr = halves(thr[2 * i : 2 * i + 1], thr[2 * i + 1 : 2 * i + 2], (1, LANES), width)
            running = thr * running + fresh
            product = product * thr
        pay_ref[i, :state, :] = running.astype(BF16)
        pay_ref[i, state:, :] = split(product)


def state_kernel(rate_any, dt_any, resets_any, b_any, c_any, x_any, *refs, width):
    pay_refs, shared, scratch = refs[: RING - 1], refs[RING - 1 : RING + 10], refs[RING + 10 :]
    start_ref, reach_ref, b_ref, c_ref, count_ref, cum_ref, scale_ref, x_ref, w_ref, bt_ref, thr_ref = shared
    rate_s, dt_s, resets_s, x_s, sems = scratch
    blocks, _, channels = start_ref.shape
    wide = channels // RING
    quarters = [where_am_i()[1] ^ k for k in range(RING)]
    at = lambda q: pl.ds(pl.multiple_of(q * wide, wide), wide)
    moves = [(dt_any, dt_s), (resets_any, resets_s), (rate_any, rate_s), (b_any, b_ref)]
    moves += [(x_any.at[:, at(q)], x_s.at[k]) for k, q in enumerate(quarters[1:])]
    moves += [(x_any.at[:, at(quarters[0])], x_ref), (c_any, c_ref)]
    copies = fetch(sems, moves)
    for copy in copies[:3]:
        copy.wait()
    scale, cum, count = prep(dt_s[...], rate_s[...], resets_s[...])
    scale_ref[...], cum_ref[...], count_ref[...] = scale, cum, count
    heads = cum.shape[0]
    for b in range(blocks):
        cols = slice(b * SPAN, (b + 1) * SPAN)
        c, n = cum[:, cols], count[:1, cols]
        end, last = c[:, SPAN - 1 :], n[:, SPAN - 1 :]
        w_ref[:, cols] = jnp.where(n == last, jnp.exp2(end - c), 0.0) * scale[:, cols]
        through = jnp.where(last == 0.0, jnp.exp2(end), 0.0)
        thr_ref[:, b * LANES : (b + 1) * LANES] = jnp.broadcast_to(through, (heads, LANES))
    copies[3].wait()
    bt_ref[...] = b_ref[...].astype(F32).T
    for k, quarter in enumerate(quarters[1:]):
        copies[4 + k].wait()
        quarter_states(quarter, x_s.at[k], pay_refs[k], start_ref, reach_ref, w_ref, bt_ref, thr_ref, width)
    for copy in copies[RING + 3 :]:
        copy.wait()


def table_kernel(skip_any, start_in, reach_in, count_ref, cum_ref, scale_ref, x_ref, w_ref, bt_ref, thr_ref, *refs, width):
    pay_ref, start_ref, reach_ref, row_ref, flip_ref, skip_ref, skip_s, sems = refs
    blocks = start_ref.shape[0]
    copies = fetch(sems, [(skip_any, skip_s)])
    quarter_states(where_am_i()[1], x_ref, pay_ref, start_ref, reach_ref, w_ref, bt_ref, thr_ref, width)
    cum, count = cum_ref[...], count_ref[...]
    heads = cum.shape[0]
    row_ref[...] = cum - jnp.log2(scale_ref[...])
    start = jnp.where(count[:1] == 0.0, jnp.exp2(cum), 0.0)
    for b in range(blocks):
        cols = slice(b * SPAN, (b + 1) * SPAN)
        stack = [cum[:, cols], start[:, cols], count[:, cols], jnp.zeros((LANES - 2 * heads - 8, SPAN), F32)]
        flip_ref[b] = jnp.concatenate(stack, axis=0).T
    copies[0].wait()
    skip_ref[...] = jnp.broadcast_to(column_of(skip_s[...]), (heads, LANES))


def split(product):
    high = product.astype(BF16).astype(F32)
    mid = (product - high).astype(BF16).astype(F32)
    low = product - high - mid
    row = lax.broadcasted_iota(jnp.int32, (TAIL, LANES), 0)
    tail = jnp.where(row == 0, high, jnp.where(row == 1, mid, jnp.where(row == 2, low, 0.0)))
    return tail.astype(BF16)


def joined(tail):
    tail = tail.astype(F32)
    return tail[0:1] + tail[1:2] + tail[2:3]


VECTORS = pl.BlockSpec(memory_space=pltpu.VMEM)
ANYWHERE = pl.BlockSpec(memory_space=pl.ANY)


def states(dt, rate, resets, bmat, cmat, xs, blocks, width):
    tokens, channels = xs.shape
    heads, state = dt.shape[0], bmat.shape[1]
    wide = channels // RING
    pay = (wide // LANES, state + TAIL, LANES)
    return pl.pallas_call(
        functools.partial(state_kernel, width=width),
        in_specs=[ANYWHERE] * 6,
        out_specs=[VECTORS] * (RING + 10),
        scratch_shapes=[
            pltpu.VMEM((1, heads), F32),
            pltpu.VMEM((heads, tokens), jnp.int32),
            pltpu.VMEM((1, tokens), jnp.int32),
            pltpu.VMEM((RING - 1, tokens, wide), BF16),
            pltpu.SemaphoreType.DMA((RING + 5,)),
        ],
        out_shape=[
            *[jax.ShapeDtypeStruct(pay, BF16)] * (RING - 1),
            jax.ShapeDtypeStruct((blocks, state, channels), BF16),
            jax.ShapeDtypeStruct((blocks, 8, channels), F32),
            jax.ShapeDtypeStruct((tokens, state), BF16),
            jax.ShapeDtypeStruct((tokens, state), BF16),
            jax.ShapeDtypeStruct((8, tokens), F32),
            jax.ShapeDtypeStruct((heads, tokens), F32),
            jax.ShapeDtypeStruct((heads, tokens), F32),
            jax.ShapeDtypeStruct((tokens, wide), BF16),
            jax.ShapeDtypeStruct((heads, tokens), F32),
            jax.ShapeDtypeStruct((state, tokens), F32),
            jax.ShapeDtypeStruct((heads, blocks * LANES), F32),
        ],
        cost_estimate=pl.CostEstimate(flops=3 * tokens * channels * state, bytes_accessed=4 << 20, transcendentals=tokens * heads),
        compiler_params=PARAMS,
        name="states",
    )(rate, dt, resets, bmat, cmat, xs)


def tables_of(skip, starts, reach, count, cum, scale, x, w, bt, thr, width):
    heads, tokens = cum.shape
    blocks, state, _ = starts.shape
    pay = (x.shape[1] // LANES, state + TAIL, LANES)
    shape = lambda a: jax.ShapeDtypeStruct(a.shape, a.dtype)
    return pl.pallas_call(
        functools.partial(table_kernel, width=width),
        in_specs=[ANYWHERE] + [VECTORS] * 9,
        out_specs=[VECTORS] * 6,
        scratch_shapes=[pltpu.VMEM((1, heads), F32), pltpu.SemaphoreType.DMA((1,))],
        out_shape=[
            jax.ShapeDtypeStruct(pay, BF16),
            shape(starts),
            shape(reach),
            shape(cum),
            jax.ShapeDtypeStruct((blocks, SPAN, LANES), F32),
            jax.ShapeDtypeStruct((heads, LANES), F32),
        ],
        input_output_aliases={1: 1, 2: 2},
        cost_estimate=pl.CostEstimate(flops=tokens * x.shape[1] * state * 4, bytes_accessed=4 << 20, transcendentals=tokens * heads),
        compiler_params=PARAMS,
        name="tables",
    )(skip, starts, reach, count, cum, scale, x, w, bt, thr)


def swapped(items, mine):
    a, b, c, d = items
    odd, high = mine % 2 == 1, mine // 2 == 1
    a, b, c, d = jnp.where(odd, b, a), jnp.where(odd, a, b), jnp.where(odd, d, c), jnp.where(odd, c, d)
    return jnp.where(high, c, a), jnp.where(high, d, b), jnp.where(high, a, c), jnp.where(high, b, d)


def prefix_kernel(*refs):
    pays, (total_ref, before_ref, reach_ref) = refs[:RING], refs[RING:]
    pairs, rows, _ = total_ref.shape
    state = rows - TAIL
    mine = where_am_i()[1]
    for i in range(pairs):
        items = swapped([p[i].astype(F32) for p in pays], mine)
        running = jnp.zeros((state, LANES), F32)
        product = jnp.ones((1, LANES), F32)
        before, reach = [], []
        for item in items:
            before.append(running)
            reach.append(jnp.broadcast_to(product, (8, LANES)))
            decay = joined(item[state:])
            running = decay * running + item[:state]
            product = decay * product
        for k, (first, second) in enumerate(zip(swapped(before, mine), swapped(reach, mine))):
            before_ref[k, i] = first
            reach_ref[k, i] = second
        total_ref[i, :state, :] = running.astype(BF16)
        total_ref[i, state:, :] = split(product)


def prefix(pays):
    pairs, rows, _ = pays[0].shape
    return pl.pallas_call(
        prefix_kernel,
        in_specs=[VECTORS] * RING,
        out_shape=[
            jax.ShapeDtypeStruct((pairs, rows, LANES), BF16),
            jax.ShapeDtypeStruct((RING, pairs, rows - TAIL, LANES), F32),
            jax.ShapeDtypeStruct((RING, pairs, 8, LANES), F32),
        ],
        cost_estimate=pl.CostEstimate(flops=1 << 20, bytes_accessed=1 << 19, transcendentals=0),
        compiler_params=PARAMS,
        name="prefix",
    )(*pays)


def spread_kernel(left_ref, before_ref, reach_ref, *outs, always):
    for k, out_ref in enumerate(outs):
        for i in range(out_ref.shape[0]):
            left = left_ref[i, : out_ref.shape[1], :].astype(F32)
            if not always:
                left = jnp.where(where_am_i()[2] % 2 == 1, left, 0.0)
            out_ref[i] = (before_ref[k, i] + reach_ref[k, i, 0:1, :] * left).astype(BF16)


def spread(left, before, reach, always):
    shape = before.shape[1:]
    vmem = pl.BlockSpec(memory_space=pltpu.VMEM)
    return pl.pallas_call(
        functools.partial(spread_kernel, always=always),
        in_specs=[vmem, vmem, vmem],
        out_shape=[jax.ShapeDtypeStruct(shape, BF16)] * RING,
        cost_estimate=pl.CostEstimate(flops=1 << 20, bytes_accessed=1 << 19, transcendentals=0),
        compiler_params=PARAMS,
        name="spread",
    )(left, before, reach)


def across(total, rings):
    state = total.shape[1] - TAIL
    shards = RING * rings
    level, send, gone, reach = 1, total, None, None
    while level < rings:
        got = lax.ppermute(send, "seq", [(i, i ^ (RING * level)) for i in range(shards)])
        if rings == 2:
            return got
        later = (where_am_i()[2] // level) % 2 == 1
        wide = lambda a: (a[:, :state].astype(F32), a[:, state : state + 3].astype(F32).sum(axis=1, keepdims=True))
        (mine, mine_p), (other, other_p) = wide(send), wide(got)
        if gone is None:
            gone, reach = jnp.zeros_like(mine), jnp.ones_like(mine_p)
        gone = jnp.where(later, gone + reach * other, gone)
        reach = jnp.where(later, reach * other_p, reach)
        both = jnp.where(later, mine + mine_p * other, other + other_p * mine)
        tail = (mine_p * other_p).astype(F32)
        high = lax.reduce_precision(tail, 8, 7)
        mid = lax.reduce_precision(tail - high, 8, 7)
        low = tail - high - mid
        rest = jnp.zeros((tail.shape[0], TAIL - 3, LANES), F32)
        send = jnp.concatenate([both, high, mid, low, rest], axis=1).astype(BF16)
        level *= 2
    pad = jnp.zeros((gone.shape[0], TAIL, LANES), F32)
    return jnp.concatenate([gone, pad], axis=1).astype(BF16)


def intra_kernel(skip_ref, b_ref, c_ref, row_ref, count_ref, flip_ref, x_any, g_any, w_any, *refs, k, teams, which, width):
    *outs, x_ref, g_ref, sems = refs
    base_ref, carry_ref = outs[:2]
    block = block_of(where_am_i(), k, teams, which)
    at = pl.ds(pl.multiple_of(block * SPAN, SPAN), SPAN)
    wide = x_ref.shape[1] // RING
    moves = []
    for i in range(RING):
        lanes = slice(i * wide, (i + 1) * wide)
        moves += [(x_any.at[at, lanes], x_ref.at[:, lanes]), (g_any.at[at, lanes], g_ref.at[:, lanes])]
    for out in outs[2:]:
        moves.append((w_any.at[:, : out.shape[1]], out))
    copies = fetch(sems, moves)
    rows, count, flipped = row_ref[:, at], count_ref[:, at], flip_ref[block]
    heads = rows.shape[0]
    dots = lax.dot_general(c_ref[at, :], b_ref[at, :], (((1,), (1,)), ((), ())), preferred_element_type=F32)
    i = lax.broadcasted_iota(jnp.int32, (SPAN, SPAN), 0)
    j = lax.broadcasted_iota(jnp.int32, (SPAN, SPAN), 1)
    linked = (flipped[:, 2 * heads : 2 * heads + 1] == count[:1]) & (j <= i)
    dots = jnp.where(linked, dots, 0.0)
    for pair in range(heads // 2):
        lanes = slice(pair * LANES, (pair + 1) * LANES)
        if pair * LANES % wide == 0:
            for copy in copies[2 * (pair * LANES // wide) :][:2]:
                copy.wait()
        x = x_ref[:, lanes]
        left, right = [], []
        for k in range(2):
            h = 2 * pair + k
            gap = jnp.minimum(flipped[:, h : h + 1] - rows[h : h + 1], 0.0)
            left.append((jnp.exp2(gap) * dots).astype(BF16))
            zero = jnp.zeros_like(x)
            right.append(halves(x, zero, x.shape, width) if k == 0 else halves(zero, x, x.shape, width))
        intra = jnp.dot(jnp.concatenate(left, axis=1), jnp.concatenate(right, axis=0), preferred_element_type=F32)
        weight = halves(skip_ref[2 * pair : 2 * pair + 1], skip_ref[2 * pair + 1 : 2 * pair + 2], (1, LANES), width)
        gate = g_ref[:, lanes].astype(F32)
        gate = gate / (1.0 + jnp.exp(-gate))
        base_ref[:, lanes] = (intra + weight * x.astype(F32)) * gate
        h = heads + 2 * pair
        carry = halves(flipped[:, h : h + 1], flipped[:, h + 1 : h + 2], x.shape, width)
        carry_ref[:, lanes] = (carry * gate).astype(BF16)
    for copy in copies[2 * RING :]:
        copy.wait()


def intra(k, teams, which, tables, xs, gate, weight, columns, width):
    channels = xs.shape[1]
    heads = tables[0].shape[0]
    extra = [jax.ShapeDtypeStruct((weight.shape[0], columns), BF16)] if columns else []
    return pl.pallas_call(
        functools.partial(intra_kernel, k=k, teams=teams, which=which, width=width),
        in_specs=[VECTORS] * 6 + [ANYWHERE] * 3,
        out_specs=[VECTORS] * (2 + len(extra)),
        scratch_shapes=[
            pltpu.VMEM((SPAN, channels), BF16),
            pltpu.VMEM((SPAN, channels), BF16),
            pltpu.SemaphoreType.DMA((2 * RING + len(extra),)),
        ],
        out_shape=[jax.ShapeDtypeStruct((SPAN, channels), F32), jax.ShapeDtypeStruct((SPAN, channels), BF16), *extra],
        cost_estimate=pl.CostEstimate(
            flops=8 * SPAN * SPAN * channels, bytes_accessed=2 << 20, transcendentals=heads * SPAN * SPAN
        ),
        compiler_params=PARAMS,
        name="intra",
    )(*tables, xs, gate, weight)


def finish_kernel(base_ref, carry_ref, c_ref, start_ref, reach_ref, gain_ref, *refs, k, teams, which):
    place_ref = where_am_i()
    in_refs, (hid_ref, sq_ref) = refs[:RING], refs[RING:]
    block = block_of(place_ref, k, teams, which)
    query = c_ref[pl.ds(pl.multiple_of(block * SPAN, SPAN), SPAN), :]
    pairs = in_refs[0].shape[0]
    wide = pairs * LANES
    total = jnp.zeros((SPAN, LANES), F32)
    quarters = [jnp.concatenate([r[i] for i in range(pairs)], axis=1).astype(F32) for r in in_refs]
    for q, incoming in enumerate(swapped(quarters, place_ref[1])):
        lanes = slice(q * wide, (q + 1) * wide)
        full = start_ref[block, :, lanes].astype(F32) + reach_ref[block, 0:1, lanes] * incoming
        inter = jnp.dot(query, full.astype(BF16), preferred_element_type=F32)
        gated = base_ref[:, lanes] + carry_ref[:, lanes].astype(F32) * inter
        square = gated * gated
        for i in range(pairs):
            total = total + square[:, i * LANES : (i + 1) * LANES]
        hid_ref[:, lanes] = (gated * gain_ref[0:1, lanes]).astype(BF16)
    sums = jnp.sum(total.T, axis=0, keepdims=True)
    sq_ref[...] = jnp.broadcast_to(sums, (8, SPAN))


def finish(k, teams, which, locals_, cmat, starts, reach, gain, incoming):
    channels = gain.shape[1]
    state = incoming[0].shape[1]
    return pl.pallas_call(
        functools.partial(finish_kernel, k=k, teams=teams, which=which),
        in_specs=[VECTORS] * (6 + RING),
        out_specs=[VECTORS] * 2,
        out_shape=[
            jax.ShapeDtypeStruct((SPAN, channels), BF16),
            jax.ShapeDtypeStruct((8, SPAN), F32),
        ],
        cost_estimate=pl.CostEstimate(flops=2 * SPAN * state * channels, bytes_accessed=3 << 20, transcendentals=0),
        compiler_params=PARAMS,
        name="finish",
    )(*locals_, cmat, starts, reach, gain, *incoming)


def product_kernel(*refs, count):
    wa, wb = refs[2 * count][...], refs[2 * count + 1][...]
    for i in range(count):
        total = jnp.dot(refs[2 * i][...], wa, preferred_element_type=F32)
        total = total + jnp.dot(refs[2 * i + 1][...], wb, preferred_element_type=F32)
        out_ref = refs[2 * count + 2 + i]
        out_ref[...] = total.astype(out_ref.dtype)


def product(lefts, dtypes, wa, wb, first, columns, tile):
    rows, depth = lefts[0][0].shape
    count = len(lefts)
    left = pl.BlockSpec((rows, depth), lambda i: (0, 0))
    right = pl.BlockSpec((depth, tile), lambda i: (0, first // tile + i))
    return pl.pallas_call(
        functools.partial(product_kernel, count=count),
        grid=(columns // tile,),
        in_specs=[left, left] * count + [right, right],
        out_specs=[pl.BlockSpec((rows, tile), lambda i: (0, i))] * count,
        out_shape=[jax.ShapeDtypeStruct((rows, columns), dtype) for dtype in dtypes],
        cost_estimate=pl.CostEstimate(
            flops=4 * count * rows * depth * columns, bytes_accessed=4 * depth * columns, transcendentals=0
        ),
        compiler_params=PARAMS,
        name="product",
    )(*(a for pair in lefts for a in pair), wa, wb)


def first_kernel(a_ref, b_ref, wa_ref, wb_any, out_ref, w_s, sems, *, step):
    depth, columns = w_s.shape
    parts = [slice(i, i + step) for i in range(0, depth, step)]
    copies = fetch(sems, [(wb_any.at[part, :columns], w_s.at[part]) for part in parts])
    total = jnp.dot(a_ref[...], wa_ref[...], preferred_element_type=F32)
    for copy, part in zip(copies, parts):
        copy.wait()
        total = total + jnp.dot(b_ref[:, part], w_s[part], preferred_element_type=F32)
    out_ref[...] = total.astype(out_ref.dtype)


def first_product(a, b, wa, wb, step=512):
    rows, depth = a.shape
    columns = wa.shape[1]
    return pl.pallas_call(
        functools.partial(first_kernel, step=step),
        in_specs=[VECTORS] * 3 + [ANYWHERE],
        out_specs=VECTORS,
        out_shape=jax.ShapeDtypeStruct((rows, columns), BF16),
        scratch_shapes=[pltpu.VMEM((depth, columns), BF16), pltpu.SemaphoreType.DMA((depth // step,))],
        cost_estimate=pl.CostEstimate(flops=4 * rows * depth * columns, bytes_accessed=4 * depth * columns, transcendentals=0),
        compiler_params=PARAMS,
        name="first",
    )(a, b, wa, wb)


def close(square, own, parts, inner, out, first, columns, shape, step=256):
    rows = shape[0]

    def body(*refs):
        sq_ref, own_ref = refs[:2]
        part_refs = refs[2 : 2 + len(parts)]
        out_any, made_s, sems = refs[-3:]
        row = lax.rsqrt(sq_ref[...] / inner + 1e-05).T[:, 0:1]
        copies = []
        for i in range(columns // step):
            here = slice(i * step, (i + 1) * step)
            total = own_ref[:, here]
            for part in part_refs:
                total = total + part[:, here].astype(F32)
            made_s[:, here] = (total * row).astype(BF16)
            there = slice(first + i * step, first + (i + 1) * step)
            copies.append(pltpu.make_async_copy(made_s.at[:, here], out_any.at[:, there], sems.at[i]))
            copies[-1].start()
        for copy in copies:
            copy.wait()

    args = [square, own, *parts]
    in_specs = [VECTORS] * len(args)
    aliases = {}
    if out is not None:
        in_specs.append(ANYWHERE)
        args.append(out)
        aliases = {len(args) - 1: 0}
    return pl.pallas_call(
        body,
        in_specs=in_specs,
        out_specs=ANYWHERE,
        out_shape=jax.ShapeDtypeStruct(shape, BF16),
        scratch_shapes=[pltpu.VMEM((rows, columns), BF16), pltpu.SemaphoreType.DMA((columns // step,))],
        input_output_aliases=aliases,
        cost_estimate=pl.CostEstimate(flops=4 * rows * columns, bytes_accessed=8 * rows * columns, transcendentals=0),
        compiler_params=PARAMS,
        name="close",
    )(*args)


def local(xs, gate, bmat, cmat, dt, resets, decay_rate, skip, gain, weight, *, shards, group):
    tokens, channels = xs.shape
    heads = dt.shape[0]
    width = channels // heads
    blocks = tokens // SPAN
    inner = float(group * channels)
    out_columns = weight.shape[1]
    teams = group // 2
    rings = shards // RING

    swap = [(i, i ^ 1) for i in range(group)]
    unit = out_columns // sum(CUTS)
    raw = weight
    held = (xs, gate, bmat, cmat, dt, weight, decay_rate[None, :], skip[None, :], resets[None, :])
    held = [pltpu.with_memory_space_constraint(a, pltpu.HBM) for a in held]
    xs, gate, bmat, cmat, dt, weight, decay_rate, skip, flags = held
    gains = gain[None, :]

    def after(value, *others):
        return lax.optimization_barrier((value, *others))[0]

    def inside(k, which, when):
        columns = CUTS[0] * unit if (k, which) == (1, 0) else 0
        return intra(k, teams, which, (when, *tables), xs, gate, weight, columns, width)

    def around(items):
        got = [items[0]]
        for k in range(1, RING):
            got.append(lax.ppermute(items[k], "seq", [(i, i ^ k) for i in range(shards)]))
        return got

    *pays, starts, reach, keys, queries, count, cum, scale, x, w, bt, thr = states(
        dt, decay_rate, flags, bmat, cmat, xs, blocks, width
    )
    first, starts, reach, row, flip, direct = tables_of(
        after(skip, pays[0]), starts, reach, count, cum, scale, x, w, bt, thr, width
    )
    tables = (keys, queries, row, count, flip)
    weight_b = lax.ppermute(after(raw, pays[0]), "head", swap)
    gathered = around([first, *pays])
    locals_ = {}
    total, before, ahead = prefix(gathered)
    left = across(total, rings)
    early = after(direct, total)
    for k in range(1, teams):
        locals_[k, 1] = inside(k, 1, early)
    outgoing = spread(left, before, ahead, rings > 2)
    incoming = around(outgoing)
    early = after(direct, outgoing[0])
    for k in range(1, teams):
        locals_[k, 0] = inside(k, 0, early)
    *locals_[1, 0], ready = locals_[1, 0]

    def pair_of(k, when):
        done = []
        late = after(gains, when)
        for which in (1, 0):
            if (k, which) not in locals_:
                locals_[k, which] = inside(k, which, when)
            hidden, sq = finish(k, teams, which, locals_[k, which], queries, starts, reach, late, incoming)
            done.append((hidden, sq))
        other = lax.ppermute(done[0][0], "head", swap)
        square = done[1][1] + lax.ppermute(done[0][1], "head", swap)
        return done[1][0], other, square

    places = [sum(CUTS[:c]) * unit for c in range(len(CUTS) + 1)]
    received = [[] for _ in CUTS]
    squares = []
    owns = {}
    mine, last = None, direct
    for k in range(1, teams):
        hidden, other, square = pair_of(k, last)
        send = [(i, (i + 2 * k) % group) for i in range(group)]
        squares.append(lax.ppermute(square, "head", send))
        for c, n in enumerate(CUTS):
            if c == ALONE and mine is None:
                *mine, square = pair_of(0, last)
                squares.append(square)
            both = c >= ALONE and k == 1
            if c == 0:
                made = [first_product(hidden, other, ready, weight_b)]
            else:
                made = product(
                    [(hidden, other), mine] if both else [(hidden, other)],
                    [BF16, F32] if both else [BF16],
                    weight,
                    weight_b,
                    places[c],
                    n * unit,
                    unit,
                )
            hidden, made = lax.optimization_barrier((hidden, made))
            if both:
                owns[c] = made[1]
            received[c].append(lax.ppermute(made[0], "head", send))
            last = after(direct, made[0])
    mine, _ = lax.optimization_barrier((mine, made[0]))
    early = product([mine], [F32], weight, weight_b, 0, places[ALONE], places[ALONE] // 3)[0]
    square = sum(squares[1:], squares[0])
    out = None
    for c, n in enumerate(CUTS):
        own = early[:, places[c] : places[c + 1]] if c < ALONE else owns[c]
        out = close(square, own, received[c], inner, out, places[c], n * unit, (SPAN, out_columns))
        if c + 1 < len(CUTS):
            out, received[c + 1] = lax.optimization_barrier((out, received[c + 1]))
    return out


def solution(mesh):
    in_specs = (
        P("seq", "head"),
        P("seq", "head"),
        P("seq", None),
        P("seq", None),
        P("head", "seq"),
        P("seq"),
        P("head"),
        P("head"),
        P("head"),
        P("head", None),
    )
    out_specs = P(("seq", "head"), None)
    body = functools.partial(local, shards=mesh.shape["seq"], group=mesh.shape["head"])

    return jax.shard_map(body, mesh=mesh, in_specs=in_specs, out_specs=out_specs, check_vma=False)
```

```python
import functools

import jax
import jax.numpy as jnp
from jax import lax
from jax.experimental import pallas as pl
from jax.experimental.pallas import tpu as pltpu
from jax.sharding import PartitionSpec as P


SPAN = 256
LANES = 128
LOG2E = 1.4426950408889634
F32 = jnp.float32
BF16 = jnp.bfloat16
PARAMS = pltpu.CompilerParams(vmem_limit_bytes=24 << 20)
WHOLE = pltpu.CompilerParams(vmem_limit_bytes=60 * 1024 * 1024)
CUTS = (2, 4, 3, 3, 3, 1)
ALONE = 3
TAIL = 8
RING = 4


def block_of(place, k, teams, i):
    team = (place[0] // 2 + k) % teams
    half = place[0] % 2
    return 2 * team + (half if i == 0 else 1 - half)


def block_cumsum(v):
    pos = lax.broadcasted_iota(jnp.int32, v.shape, 1) % SPAN
    k = 1
    while k < SPAN:
        v = v + jnp.where(pos >= k, pltpu.roll(v, k, 1), 0.0)
        k *= 2
    return v


def column_of(row):
    n = row.shape[1]
    at = lax.broadcasted_iota(jnp.int32, (n, n), 0) == lax.broadcasted_iota(jnp.int32, (n, n), 1)
    return jnp.sum(jnp.where(at, jnp.broadcast_to(row, (n, n)), 0.0), axis=1, keepdims=True)


def where_am_i():
    shard = lax.axis_index("seq")
    return lax.axis_index("head"), shard & (RING - 1), shard >> (RING.bit_length() - 1)


def prep(dt, rate, resets):
    step = dt.astype(F32) / 16.0
    scale = jnp.minimum(step, 1.0)
    cum = block_cumsum((-LOG2E * column_of(rate)) * step)
    count = block_cumsum(jnp.broadcast_to(resets.astype(F32), (8, resets.shape[1])))
    return scale, cum, count


def halves(first, second, shape, width):
    lane = lax.broadcasted_iota(jnp.int32, shape, 1) % LANES
    return jnp.where(lane < width, first, second)


def fetch(sems, pairs):
    copies = [pltpu.make_async_copy(src, dst, sems.at[i]) for i, (src, dst) in enumerate(pairs)]
    for copy in copies:
        copy.start()
    return copies


def fetch(sems, pairs):
    copies = [pltpu.make_async_copy(src, dst, sems.at[i]) for i, (src, dst) in enumerate(pairs)]
    for copy in copies:
        copy.start()
    return copies


def quarter_states(quarter, x_ref, pay_ref, start_ref, reach_ref, w_ref, bt_ref, thr_ref, width):
    blocks, state, channels = start_ref.shape
    wide = channels // RING
    pairs = wide // LANES
    two = 4 * pairs
    own = pl.ds(pl.multiple_of(quarter // 2 * two, two), two)
    odd = quarter % 2 == 1

    def rows_of(ref, cols):
        both = ref[own, cols]
        return jnp.where(odd, both[two // 2 :], both[: two // 2])

    for i in range(pairs):
        lanes = pl.ds(pl.multiple_of(quarter * wide + i * LANES, LANES), LANES)
        running = jnp.zeros((state, LANES), F32)
        product = jnp.ones((1, LANES), F32)
        for b in range(blocks):
            cols = slice(b * SPAN, (b + 1) * SPAN)
            start_ref[b, :, lanes] = running.astype(BF16)
            reach_ref[b, :, lanes] = jnp.broadcast_to(product, (8, LANES))
            x = x_ref[cols, i * LANES : (i + 1) * LANES]
            rows = rows_of(w_ref, cols)
            parts = []
            for j in range(2):
                left = (bt_ref[:, cols] * rows[2 * i + j : 2 * i + j + 1]).astype(BF16)
                parts.append(jnp.dot(left, x, preferred_element_type=F32))
            fresh = halves(parts[0], parts[1], (state, LANES), width)
            thr = rows_of(thr_ref, slice(b * LANES, (b + 1) * LANES))
            thr = halves(thr[2 * i : 2 * i + 1], thr[2 * i + 1 : 2 * i + 2], (1, LANES), width)
            running = thr * running + fresh
            product = product * thr
        pay_ref[i, :state, :] = running.astype(BF16)
        pay_ref[i, state:, :] = split(product)


def state_kernel(rate_any, dt_any, resets_any, b_any, c_any, x_any, *refs, width):
    pay_refs, shared, scratch = refs[: RING - 1], refs[RING - 1 : RING + 10], refs[RING + 10 :]
    start_ref, reach_ref, b_ref, c_ref, count_ref, cum_ref, scale_ref, x_ref, w_ref, bt_ref, thr_ref = shared
    rate_s, dt_s, resets_s, x_s, sems = scratch
    blocks, _, channels = start_ref.shape
    wide = channels // RING
    quarters = [where_am_i()[1] ^ k for k in range(RING)]
    at = lambda q: pl.ds(pl.multiple_of(q * wide, wide), wide)
    moves = [(dt_any, dt_s), (resets_any, resets_s), (rate_any, rate_s), (b_any, b_ref)]
    moves += [(x_any.at[:, at(q)], x_s.at[k]) for k, q in enumerate(quarters[1:])]
    moves += [(x_any.at[:, at(quarters[0])], x_ref), (c_any, c_ref)]
    copies = fetch(sems, moves)
    for copy in copies[:3]:
        copy.wait()
    scale, cum, count = prep(dt_s[...], rate_s[...], resets_s[...])
    scale_ref[...], cum_ref[...], count_ref[...] = scale, cum, count
    heads = cum.shape[0]
    for b in range(blocks):
        cols = slice(b * SPAN, (b + 1) * SPAN)
        c, n = cum[:, cols], count[:1, cols]
        end, last = c[:, SPAN - 1 :], n[:, SPAN - 1 :]
        w_ref[:, cols] = jnp.where(n == last, jnp.exp2(end - c), 0.0) * scale[:, cols]
        through = jnp.where(last == 0.0, jnp.exp2(end), 0.0)
        thr_ref[:, b * LANES : (b + 1) * LANES] = jnp.broadcast_to(through, (heads, LANES))
    copies[3].wait()
    bt_ref[...] = b_ref[...].astype(F32).T
    for k, quarter in enumerate(quarters[1:]):
        copies[4 + k].wait()
        quarter_states(quarter, x_s.at[k], pay_refs[k], start_ref, reach_ref, w_ref, bt_ref, thr_ref, width)
    for copy in copies[RING + 3 :]:
        copy.wait()


def table_kernel(skip_any, start_in, reach_in, count_ref, cum_ref, scale_ref, x_ref, w_ref, bt_ref, thr_ref, *refs, width):
    pay_ref, start_ref, reach_ref, row_ref, flip_ref, skip_ref, skip_s, sems = refs
    blocks = start_ref.shape[0]
    copies = fetch(sems, [(skip_any, skip_s)])
    quarter_states(where_am_i()[1], x_ref, pay_ref, start_ref, reach_ref, w_ref, bt_ref, thr_ref, width)
    cum, count = cum_ref[...], count_ref[...]
    heads = cum.shape[0]
    row_ref[...] = cum - jnp.log2(scale_ref[...])
    start = jnp.where(count[:1] == 0.0, jnp.exp2(cum), 0.0)
    for b in range(blocks):
        cols = slice(b * SPAN, (b + 1) * SPAN)
        stack = [cum[:, cols], start[:, cols], count[:, cols], jnp.zeros((LANES - 2 * heads - 8, SPAN), F32)]
        flip_ref[b] = jnp.concatenate(stack, axis=0).T
    copies[0].wait()
    skip_ref[...] = jnp.broadcast_to(column_of(skip_s[...]), (heads, LANES))


def split(product):
    high = product.astype(BF16).astype(F32)
    mid = (product - high).astype(BF16).astype(F32)
    low = product - high - mid
    row = lax.broadcasted_iota(jnp.int32, (TAIL, LANES), 0)
    tail = jnp.where(row == 0, high, jnp.where(row == 1, mid, jnp.where(row == 2, low, 0.0)))
    return tail.astype(BF16)


def joined(tail):
    tail = tail.astype(F32)
    return tail[0:1] + tail[1:2] + tail[2:3]


VECTORS = pl.BlockSpec(memory_space=pltpu.VMEM)
ANYWHERE = pl.BlockSpec(memory_space=pl.ANY)


def states(dt, rate, resets, bmat, cmat, xs, blocks, width):
    tokens, channels = xs.shape
    heads, state = dt.shape[0], bmat.shape[1]
    wide = channels // RING
    pay = (wide // LANES, state + TAIL, LANES)
    return pl.pallas_call(
        functools.partial(state_kernel, width=width),
        in_specs=[ANYWHERE] * 6,
        out_specs=[VECTORS] * (RING + 10),
        scratch_shapes=[
            pltpu.VMEM((1, heads), F32),
            pltpu.VMEM((heads, tokens), jnp.int32),
            pltpu.VMEM((1, tokens), jnp.int32),
            pltpu.VMEM((RING - 1, tokens, wide), BF16),
            pltpu.SemaphoreType.DMA((RING + 5,)),
        ],
        out_shape=[
            *[jax.ShapeDtypeStruct(pay, BF16)] * (RING - 1),
            jax.ShapeDtypeStruct((blocks, state, channels), BF16),
            jax.ShapeDtypeStruct((blocks, 8, channels), F32),
            jax.ShapeDtypeStruct((tokens, state), BF16),
            jax.ShapeDtypeStruct((tokens, state), BF16),
            jax.ShapeDtypeStruct((8, tokens), F32),
            jax.ShapeDtypeStruct((heads, tokens), F32),
            jax.ShapeDtypeStruct((heads, tokens), F32),
            jax.ShapeDtypeStruct((tokens, wide), BF16),
            jax.ShapeDtypeStruct((heads, tokens), F32),
            jax.ShapeDtypeStruct((state, tokens), F32),
            jax.ShapeDtypeStruct((heads, blocks * LANES), F32),
        ],
        cost_estimate=pl.CostEstimate(flops=3 * tokens * channels * state, bytes_accessed=4 << 20, transcendentals=tokens * heads),
        compiler_params=PARAMS,
        name="states",
    )(rate, dt, resets, bmat, cmat, xs)


def tables_of(skip, starts, reach, count, cum, scale, x, w, bt, thr, width):
    heads, tokens = cum.shape
    blocks, state, _ = starts.shape
    pay = (x.shape[1] // LANES, state + TAIL, LANES)
    shape = lambda a: jax.ShapeDtypeStruct(a.shape, a.dtype)
    return pl.pallas_call(
        functools.partial(table_kernel, width=width),
        in_specs=[ANYWHERE] + [VECTORS] * 9,
        out_specs=[VECTORS] * 6,
        scratch_shapes=[pltpu.VMEM((1, heads), F32), pltpu.SemaphoreType.DMA((1,))],
        out_shape=[
            jax.ShapeDtypeStruct(pay, BF16),
            shape(starts),
            shape(reach),
            shape(cum),
            jax.ShapeDtypeStruct((blocks, SPAN, LANES), F32),
            jax.ShapeDtypeStruct((heads, LANES), F32),
        ],
        input_output_aliases={1: 1, 2: 2},
        cost_estimate=pl.CostEstimate(flops=tokens * x.shape[1] * state * 4, bytes_accessed=4 << 20, transcendentals=tokens * heads),
        compiler_params=PARAMS,
        name="tables",
    )(skip, starts, reach, count, cum, scale, x, w, bt, thr)


def swapped(items, mine):
    a, b, c, d = items
    odd, high = mine % 2 == 1, mine // 2 == 1
    a, b, c, d = jnp.where(odd, b, a), jnp.where(odd, a, b), jnp.where(odd, d, c), jnp.where(odd, c, d)
    return jnp.where(high, c, a), jnp.where(high, d, b), jnp.where(high, a, c), jnp.where(high, b, d)


def prefix_kernel(*refs):
    pays, (total_ref, before_ref, reach_ref) = refs[:RING], refs[RING:]
    pairs, rows, _ = total_ref.shape
    state = rows - TAIL
    mine = where_am_i()[1]
    for i in range(pairs):
        items = swapped([p[i].astype(F32) for p in pays], mine)
        running = jnp.zeros((state, LANES), F32)
        product = jnp.ones((1, LANES), F32)
        before, reach = [], []
        for item in items:
            before.append(running)
            reach.append(jnp.broadcast_to(product, (8, LANES)))
            decay = joined(item[state:])
            running = decay * running + item[:state]
            product = decay * product
        for k, (first, second) in enumerate(zip(swapped(before, mine), swapped(reach, mine))):
            before_ref[k, i] = first
            reach_ref[k, i] = second
        total_ref[i, :state, :] = running.astype(BF16)
        total_ref[i, state:, :] = split(product)


def prefix(pays):
    pairs, rows, _ = pays[0].shape
    return pl.pallas_call(
        prefix_kernel,
        in_specs=[VECTORS] * RING,
        out_shape=[
            jax.ShapeDtypeStruct((pairs, rows, LANES), BF16),
            jax.ShapeDtypeStruct((RING, pairs, rows - TAIL, LANES), F32),
            jax.ShapeDtypeStruct((RING, pairs, 8, LANES), F32),
        ],
        cost_estimate=pl.CostEstimate(flops=1 << 20, bytes_accessed=1 << 19, transcendentals=0),
        compiler_params=PARAMS,
        name="prefix",
    )(*pays)


def spread_kernel(left_ref, before_ref, reach_ref, *outs, always):
    for k, out_ref in enumerate(outs):
        for i in range(out_ref.shape[0]):
            left = left_ref[i, : out_ref.shape[1], :].astype(F32)
            if not always:
                left = jnp.where(where_am_i()[2] % 2 == 1, left, 0.0)
            out_ref[i] = (before_ref[k, i] + reach_ref[k, i, 0:1, :] * left).astype(BF16)


def spread(left, before, reach, always):
    shape = before.shape[1:]
    vmem = pl.BlockSpec(memory_space=pltpu.VMEM)
    return pl.pallas_call(
        functools.partial(spread_kernel, always=always),
        in_specs=[vmem, vmem, vmem],
        out_shape=[jax.ShapeDtypeStruct(shape, BF16)] * RING,
        cost_estimate=pl.CostEstimate(flops=1 << 20, bytes_accessed=1 << 19, transcendentals=0),
        compiler_params=PARAMS,
        name="spread",
    )(left, before, reach)


def across(total, rings):
    state = total.shape[1] - TAIL
    shards = RING * rings
    level, send, gone, reach = 1, total, None, None
    while level < rings:
        got = lax.ppermute(send, "seq", [(i, i ^ (RING * level)) for i in range(shards)])
        if rings == 2:
            return got
        later = (where_am_i()[2] // level) % 2 == 1
        wide = lambda a: (a[:, :state].astype(F32), a[:, state : state + 3].astype(F32).sum(axis=1, keepdims=True))
        (mine, mine_p), (other, other_p) = wide(send), wide(got)
        if gone is None:
            gone, reach = jnp.zeros_like(mine), jnp.ones_like(mine_p)
        gone = jnp.where(later, gone + reach * other, gone)
        reach = jnp.where(later, reach * other_p, reach)
        both = jnp.where(later, mine + mine_p * other, other + other_p * mine)
        tail = (mine_p * other_p).astype(F32)
        high = lax.reduce_precision(tail, 8, 7)
        mid = lax.reduce_precision(tail - high, 8, 7)
        low = tail - high - mid
        rest = jnp.zeros((tail.shape[0], TAIL - 3, LANES), F32)
        send = jnp.concatenate([both, high, mid, low, rest], axis=1).astype(BF16)
        level *= 2
    pad = jnp.zeros((gone.shape[0], TAIL, LANES), F32)
    return jnp.concatenate([gone, pad], axis=1).astype(BF16)


def intra_kernel(skip_ref, b_ref, c_ref, row_ref, count_ref, flip_ref, x_any, g_any, w_any, *refs, k, teams, which, width):
    *outs, x_ref, g_ref, sems = refs
    base_ref, carry_ref = outs[:2]
    block = block_of(where_am_i(), k, teams, which)
    at = pl.ds(pl.multiple_of(block * SPAN, SPAN), SPAN)
    wide = x_ref.shape[1] // RING
    moves = []
    for i in range(RING):
        lanes = slice(i * wide, (i + 1) * wide)
        moves += [(x_any.at[at, lanes], x_ref.at[:, lanes]), (g_any.at[at, lanes], g_ref.at[:, lanes])]
    for out in outs[2:]:
        moves.append((w_any.at[:, : out.shape[1]], out))
    copies = fetch(sems, moves)
    rows, count, flipped = row_ref[:, at], count_ref[:, at], flip_ref[block]
    heads = rows.shape[0]
    dots = lax.dot_general(c_ref[at, :], b_ref[at, :], (((1,), (1,)), ((), ())), preferred_element_type=F32)
    i = lax.broadcasted_iota(jnp.int32, (SPAN, SPAN), 0)
    j = lax.broadcasted_iota(jnp.int32, (SPAN, SPAN), 1)
    linked = (flipped[:, 2 * heads : 2 * heads + 1] == count[:1]) & (j <= i)
    dots = jnp.where(linked, dots, 0.0)
    for pair in range(heads // 2):
        lanes = slice(pair * LANES, (pair + 1) * LANES)
        if pair * LANES % wide == 0:
            for copy in copies[2 * (pair * LANES // wide) :][:2]:
                copy.wait()
        x = x_ref[:, lanes]
        left, right = [], []
        for k in range(2):
            h = 2 * pair + k
            gap = jnp.minimum(flipped[:, h : h + 1] - rows[h : h + 1], 0.0)
            left.append((jnp.exp2(gap) * dots).astype(BF16))
            zero = jnp.zeros_like(x)
            right.append(halves(x, zero, x.shape, width) if k == 0 else halves(zero, x, x.shape, width))
        intra = jnp.dot(jnp.concatenate(left, axis=1), jnp.concatenate(right, axis=0), preferred_element_type=F32)
        weight = halves(skip_ref[2 * pair : 2 * pair + 1], skip_ref[2 * pair + 1 : 2 * pair + 2], (1, LANES), width)
        gate = g_ref[:, lanes].astype(F32)
        gate = gate / (1.0 + jnp.exp(-gate))
        base_ref[:, lanes] = (intra + weight * x.astype(F32)) * gate
        h = heads + 2 * pair
        carry = halves(flipped[:, h : h + 1], flipped[:, h + 1 : h + 2], x.shape, width)
        carry_ref[:, lanes] = (carry * gate).astype(BF16)
    for copy in copies[2 * RING :]:
        copy.wait()


def intra(k, teams, which, tables, xs, gate, weight, columns, width):
    channels = xs.shape[1]
    heads = tables[0].shape[0]
    extra = [jax.ShapeDtypeStruct((weight.shape[0], columns), BF16)] if columns else []
    return pl.pallas_call(
        functools.partial(intra_kernel, k=k, teams=teams, which=which, width=width),
        in_specs=[VECTORS] * 6 + [ANYWHERE] * 3,
        out_specs=[VECTORS] * (2 + len(extra)),
        scratch_shapes=[
            pltpu.VMEM((SPAN, channels), BF16),
            pltpu.VMEM((SPAN, channels), BF16),
            pltpu.SemaphoreType.DMA((2 * RING + len(extra),)),
        ],
        out_shape=[jax.ShapeDtypeStruct((SPAN, channels), F32), jax.ShapeDtypeStruct((SPAN, channels), BF16), *extra],
        cost_estimate=pl.CostEstimate(
            flops=8 * SPAN * SPAN * channels, bytes_accessed=2 << 20, transcendentals=heads * SPAN * SPAN
        ),
        compiler_params=PARAMS,
        name="intra",
    )(*tables, xs, gate, weight)


def finish_kernel(base_ref, carry_ref, c_ref, start_ref, reach_ref, gain_ref, *refs, k, teams, which):
    place_ref = where_am_i()
    in_refs, (hid_ref, sq_ref) = refs[:RING], refs[RING:]
    block = block_of(place_ref, k, teams, which)
    query = c_ref[pl.ds(pl.multiple_of(block * SPAN, SPAN), SPAN), :]
    pairs = in_refs[0].shape[0]
    wide = pairs * LANES
    total = jnp.zeros((SPAN, LANES), F32)
    quarters = [jnp.concatenate([r[i] for i in range(pairs)], axis=1).astype(F32) for r in in_refs]
    for q, incoming in enumerate(swapped(quarters, place_ref[1])):
        lanes = slice(q * wide, (q + 1) * wide)
        full = start_ref[block, :, lanes].astype(F32) + reach_ref[block, 0:1, lanes] * incoming
        inter = jnp.dot(query, full.astype(BF16), preferred_element_type=F32)
        gated = base_ref[:, lanes] + carry_ref[:, lanes].astype(F32) * inter
        square = gated * gated
        for i in range(pairs):
            total = total + square[:, i * LANES : (i + 1) * LANES]
        hid_ref[:, lanes] = (gated * gain_ref[0:1, lanes]).astype(BF16)
    sums = jnp.sum(total.T, axis=0, keepdims=True)
    sq_ref[...] = jnp.broadcast_to(sums, (8, SPAN))


def finish(k, teams, which, locals_, cmat, starts, reach, gain, incoming):
    channels = gain.shape[1]
    state = incoming[0].shape[1]
    return pl.pallas_call(
        functools.partial(finish_kernel, k=k, teams=teams, which=which),
        in_specs=[VECTORS] * (6 + RING),
        out_specs=[VECTORS] * 2,
        out_shape=[
            jax.ShapeDtypeStruct((SPAN, channels), BF16),
            jax.ShapeDtypeStruct((8, SPAN), F32),
        ],
        cost_estimate=pl.CostEstimate(flops=2 * SPAN * state * channels, bytes_accessed=3 << 20, transcendentals=0),
        compiler_params=PARAMS,
        name="finish",
    )(*locals_, cmat, starts, reach, gain, *incoming)


def product_kernel(*refs, count):
    wa, wb = refs[2 * count][...], refs[2 * count + 1][...]
    for i in range(count):
        total = jnp.dot(refs[2 * i][...], wa, preferred_element_type=F32)
        total = total + jnp.dot(refs[2 * i + 1][...], wb, preferred_element_type=F32)
        out_ref = refs[2 * count + 2 + i]
        out_ref[...] = total.astype(out_ref.dtype)


def product(lefts, dtypes, wa, wb, first, columns, tile):
    rows, depth = lefts[0][0].shape
    count = len(lefts)
    left = pl.BlockSpec((rows, depth), lambda i: (0, 0))
    right = pl.BlockSpec((depth, tile), lambda i: (0, first // tile + i))
    return pl.pallas_call(
        functools.partial(product_kernel, count=count),
        grid=(columns // tile,),
        in_specs=[left, left] * count + [right, right],
        out_specs=[pl.BlockSpec((rows, tile), lambda i: (0, i))] * count,
        out_shape=[jax.ShapeDtypeStruct((rows, columns), dtype) for dtype in dtypes],
        cost_estimate=pl.CostEstimate(
            flops=4 * count * rows * depth * columns, bytes_accessed=4 * depth * columns, transcendentals=0
        ),
        compiler_params=PARAMS,
        name="product",
    )(*(a for pair in lefts for a in pair), wa, wb)


def first_kernel(a_ref, b_ref, wa_ref, wb_any, out_ref, w_s, sems, *, step):
    depth, columns = w_s.shape
    parts = [slice(i, i + step) for i in range(0, depth, step)]
    copies = fetch(sems, [(wb_any.at[part, :columns], w_s.at[part]) for part in parts])
    total = jnp.dot(a_ref[...], wa_ref[...], preferred_element_type=F32)
    for copy, part in zip(copies, parts):
        copy.wait()
        total = total + jnp.dot(b_ref[:, part], w_s[part], preferred_element_type=F32)
    out_ref[...] = total.astype(out_ref.dtype)


def first_product(a, b, wa, wb, step=512):
    rows, depth = a.shape
    columns = wa.shape[1]
    return pl.pallas_call(
        functools.partial(first_kernel, step=step),
        in_specs=[VECTORS] * 3 + [ANYWHERE],
        out_specs=VECTORS,
        out_shape=jax.ShapeDtypeStruct((rows, columns), BF16),
        scratch_shapes=[pltpu.VMEM((depth, columns), BF16), pltpu.SemaphoreType.DMA((depth // step,))],
        cost_estimate=pl.CostEstimate(flops=4 * rows * depth * columns, bytes_accessed=4 * depth * columns, transcendentals=0),
        compiler_params=PARAMS,
        name="first",
    )(a, b, wa, wb)


def factor(square, inner):
    rows = square.shape[1]

    def body(sq_ref, out_ref):
        out_ref[...] = jnp.broadcast_to(lax.rsqrt(sq_ref[...] / inner + 1e-05).T[:, 0:1], (rows, LANES))

    return pl.pallas_call(
        body,
        in_specs=[VECTORS],
        out_specs=VECTORS,
        out_shape=jax.ShapeDtypeStruct((rows, LANES), F32),
        compiler_params=PARAMS,
        name="factor",
    )(square)


def close(square, own, parts, out, first, columns, shape, step=256):
    rows = shape[0]

    def body(*refs):
        sq_ref, own_ref = refs[:2]
        part_refs = refs[2 : 2 + len(parts)]
        out_any, made_s, sems = refs[-3:]
        row = jnp.concatenate([sq_ref[...]] * (step // LANES), axis=1)
        copies = []
        for i in range(columns // step):
            here = slice(i * step, (i + 1) * step)
            total = own_ref[:, here]
            for part in part_refs:
                total = total + part[:, here].astype(F32)
            made_s[:, here] = (total * row).astype(BF16)
            there = slice(first + i * step, first + (i + 1) * step)
            copies.append(pltpu.make_async_copy(made_s.at[:, here], out_any.at[:, there], sems.at[i]))
            copies[-1].start()
        for copy in copies:
            copy.wait()

    args = [square, own, *parts]
    in_specs = [VECTORS] * len(args)
    aliases = {}
    if out is not None:
        in_specs.append(ANYWHERE)
        args.append(out)
        aliases = {len(args) - 1: 0}
    return pl.pallas_call(
        body,
        in_specs=in_specs,
        out_specs=ANYWHERE,
        out_shape=jax.ShapeDtypeStruct(shape, BF16),
        scratch_shapes=[pltpu.VMEM((rows, columns), BF16), pltpu.SemaphoreType.DMA((columns // step,))],
        input_output_aliases=aliases,
        cost_estimate=pl.CostEstimate(flops=4 * rows * columns, bytes_accessed=8 * rows * columns, transcendentals=0),
        compiler_params=PARAMS,
        name="close",
    )(*args)


def local(xs, gate, bmat, cmat, dt, resets, decay_rate, skip, gain, weight, *, shards, group):
    tokens, channels = xs.shape
    heads = dt.shape[0]
    width = channels // heads
    blocks = tokens // SPAN
    inner = float(group * channels)
    out_columns = weight.shape[1]
    teams = group // 2
    rings = shards // RING

    swap = [(i, i ^ 1) for i in range(group)]
    unit = out_columns // sum(CUTS)
    raw = weight
    held = (xs, gate, bmat, cmat, dt, weight, decay_rate[None, :], skip[None, :], resets[None, :])
    held = [pltpu.with_memory_space_constraint(a, pltpu.HBM) for a in held]
    xs, gate, bmat, cmat, dt, weight, decay_rate, skip, flags = held
    gains = gain[None, :]

    def after(value, *others):
        return lax.optimization_barrier((value, *others))[0]

    def inside(k, which, when):
        columns = CUTS[0] * unit if (k, which) == (1, 0) else 0
        return intra(k, teams, which, (when, *tables), xs, gate, weight, columns, width)

    def around(items):
        got = [items[0]]
        for k in range(1, RING):
            got.append(lax.ppermute(items[k], "seq", [(i, i ^ k) for i in range(shards)]))
        return got

    *pays, starts, reach, keys, queries, count, cum, scale, x, w, bt, thr = states(
        dt, decay_rate, flags, bmat, cmat, xs, blocks, width
    )
    first, starts, reach, row, flip, direct = tables_of(
        after(skip, pays[0]), starts, reach, count, cum, scale, x, w, bt, thr, width
    )
    tables = (keys, queries, row, count, flip)
    weight_b = lax.ppermute(after(raw, pays[0]), "head", swap)
    gathered = around([first, *pays])
    locals_ = {}
    total, before, ahead = prefix(gathered)
    left = across(total, rings)
    early = after(direct, total)
    for k in range(1, teams):
        locals_[k, 1] = inside(k, 1, early)
    outgoing = spread(left, before, ahead, rings > 2)
    incoming = around(outgoing)
    early = after(direct, outgoing[0])
    for k in range(1, teams):
        locals_[k, 0] = inside(k, 0, early)
    *locals_[1, 0], ready = locals_[1, 0]

    def pair_of(k, when):
        done = []
        late = after(gains, when)
        for which in (1, 0):
            if (k, which) not in locals_:
                locals_[k, which] = inside(k, which, when)
            hidden, sq = finish(k, teams, which, locals_[k, which], queries, starts, reach, late, incoming)
            done.append((hidden, sq))
        other = lax.ppermute(done[0][0], "head", swap)
        square = done[1][1] + lax.ppermute(done[0][1], "head", swap)
        return done[1][0], other, square

    places = [sum(CUTS[:c]) * unit for c in range(len(CUTS) + 1)]
    received = [[] for _ in CUTS]
    squares = []
    owns = {}
    mine, last = None, direct
    for k in range(1, teams):
        hidden, other, square = pair_of(k, last)
        send = [(i, (i + 2 * k) % group) for i in range(group)]
        squares.append(lax.ppermute(square, "head", send))
        for c, n in enumerate(CUTS):
            if c == ALONE and mine is None:
                *mine, square = pair_of(0, last)
                squares.append(square)
            both = c >= ALONE and k == 1
            if c == 0:
                made = [first_product(hidden, other, ready, weight_b)]
            else:
                made = product(
                    [(hidden, other), mine] if both else [(hidden, other)],
                    [BF16, F32] if both else [BF16],
                    weight,
                    weight_b,
                    places[c],
                    n * unit,
                    unit,
                )
            hidden, made = lax.optimization_barrier((hidden, made))
            if both:
                owns[c] = made[1]
            received[c].append(lax.ppermute(made[0], "head", send))
            last = after(direct, made[0])
    mine, _ = lax.optimization_barrier((mine, made[0]))
    early = product([mine], [F32], weight, weight_b, 0, places[ALONE], places[ALONE] // 3)[0]
    square = factor(sum(squares[1:], squares[0]), inner)
    out = None
    for c, n in enumerate(CUTS):
        own = early[:, places[c] : places[c + 1]] if c < ALONE else owns[c]
        out = close(square, own, received[c], out, places[c], n * unit, (SPAN, out_columns))
        if c + 1 < len(CUTS):
            out, received[c + 1] = lax.optimization_barrier((out, received[c + 1]))
    return out


def solution(mesh):
    in_specs = (
        P("seq", "head"),
        P("seq", "head"),
        P("seq", None),
        P("seq", None),
        P("head", "seq"),
        P("seq"),
        P("head"),
        P("head"),
        P("head"),
        P("head", None),
    )
    out_specs = P(("seq", "head"), None)
    body = functools.partial(local, shards=mesh.shape["seq"], group=mesh.shape["head"])

    return jax.shard_map(body, mesh=mesh, in_specs=in_specs, out_specs=out_specs, check_vma=False)
```
